8 devices in a mesh: dp: 2 (over y, z), tp: 4 (over x, core).
Axes of the slice: x: 2, y: 2, z: 1, core: 2. Of those that a mesh axis runs over, the one named last changes fastest.
Arguments:
- x: bfloat16 [2048, 4096], P(('dp', 'tp')), parts along dimension 0
- dy: bfloat16 [2048, 4096], P(('dp', 'tp')), parts along dimension 0
- gain: bfloat16 [4096], replicated
- wq: bfloat16 [4096, 4096], P(None, 'tp')
- wk: bfloat16 [4096, 512], P(None, 'tp')
- wv: bfloat16 [4096, 512], P(None, 'tp')
- wo: bfloat16 [4096, 4096], P('tp')
Outputs:
- output 1: bfloat16 [2048, 4096], P(('dp', 'tp')), parts along dimension 0
- output 2: float32 [2, 4096], P('dp'), parts along dimension 0
- output 3: bfloat16 [8192, 4096], P('dp', 'tp'), parts along dimension 0
- output 4: bfloat16 [8192, 512], P('dp', 'tp'), parts along dimension 0
- output 5: bfloat16 [8192, 512], P('dp', 'tp'), parts along dimension 0
- output 6: bfloat16 [8192, 4096], P(('dp', 'tp')), parts along dimension 0
There are 2 independent parts. The reference program is written for one: setup_inputs(seed, part) draws one part's arguments, and reference() takes and returns one part's arrays. A program takes and returns all parts, laid end to end along the dimension named above; an argument that names none is the same for every part.
All inputs are finite; a program needn't handle non-finite values.
Results may differ from the reference program's by a relative error of at most 0.018.
Values are sent between devices in bfloat16 or wider.
A program may use at most 2 GiB of HBM per device.

```python
import jax
import jax.numpy as jnp
from jax import lax

ROWS = 1024
D = 4096
HEADS = 32
KV_HEADS = 4
HEAD = 128
THETA = 10000


def setup_inputs(seed: int = 0, part: int = 0) -> dict:
    kx, ky, kn, kq, kk, kv, ko = jax.random.split(jax.random.key(seed), 7)

    def weights(key, rows, columns):
        return jax.random.normal(key, (rows, columns), jnp.float32) * rows**-0.5

    drawn = {
        "x": jax.random.normal(jax.random.fold_in(kx, part), (ROWS, D), jnp.float32),
        "dy": jax.random.normal(jax.random.fold_in(ky, part), (ROWS, D), jnp.float32) * ROWS**-0.5,
        "gain": 1 + 0.1 * jax.random.normal(kn, (D,), jnp.float32),
        "wq": 2 * weights(kq, D, HEADS * HEAD),
        "wk": 2 * weights(kk, D, KV_HEADS * HEAD),
        "wv": 4 * weights(kv, D, KV_HEADS * HEAD),
        "wo": weights(ko, HEADS * HEAD, D),
    }
    return {k: v.astype(jnp.bfloat16) for k, v in drawn.items()}


def normed(x, gain):
    wide = x.astype(jnp.float32)
    scale = lax.rsqrt(jnp.mean(wide * wide, -1, keepdims=True) + 1e-6)
    return (wide * scale * gain.astype(jnp.float32)).astype(jnp.bfloat16)


def turned(t, place, theta):
    half = t.shape[-1] // 2
    angle = place.astype(jnp.float32)[:, None] * theta ** (-jnp.arange(half, dtype=jnp.float32) / half)
    cos, sin = jnp.cos(angle)[:, None], jnp.sin(angle)[:, None]
    a, b = t[..., :half].astype(jnp.float32), t[..., half:].astype(jnp.float32)
    return jnp.concatenate([a * cos - b * sin, b * cos + a * sin], -1).astype(jnp.bfloat16)


def matmul(a, w):
    return jnp.dot(a, w, preferred_element_type=jnp.float32).astype(jnp.bfloat16)


def einsum(form, a, b):
    return jnp.einsum(form, a.astype(jnp.float32), b.astype(jnp.float32))


def attention(q, k, v):
    scores = einsum("tgsd,ugd->gstu", q, k) * q.shape[-1] ** -0.5
    token = jnp.arange(q.shape[0])
    scores = jnp.where(token[:, None] >= token, scores, -jnp.inf)
    weights = jax.nn.softmax(scores, -1).astype(jnp.bfloat16)
    return einsum("gstu,ugd->tgsd", weights, v).astype(jnp.bfloat16)


def forward(x, gain, wq, wk, wv, wo):
    rows = x.shape[0]
    a, place = normed(x, gain), jnp.arange(rows)
    k = turned(matmul(a, wk).reshape(rows, -1, HEAD), place, THETA)
    q = turned(matmul(a, wq).reshape(rows, -1, HEAD), place, THETA).reshape(rows, k.shape[1], -1, HEAD)
    v = matmul(a, wv).reshape(rows, -1, HEAD)
    seen = attention(q, k, v).reshape(rows, -1)
    return (x.astype(jnp.float32) + jnp.dot(seen, wo, preferred_element_type=jnp.float32)).astype(jnp.bfloat16)


def reference(x, dy, gain, wq, wk, wv, wo):
    _, back = jax.vjp(forward, x, gain.astype(jnp.float32), wq, wk, wv, wo)
    by_x, by_gain, *by_weights = back(dy)
    return (by_x, by_gain[None], *by_weights)
```

```python
import jax
import jax.numpy as jnp
from jax import lax
from jax.experimental import pallas as pl
from jax.experimental.pallas import tpu as pltpu

NEG = -1e30
HIDDEN = 2 * NEG
LOG2E = 1.4426950408889634
VMEM = 56 * 2**20


def _dot(a, b, ca, cb):
    return lax.dot_general(a, b, (((ca,), (cb,)), ((), ())), preferred_element_type=jnp.float32)


from jax.sharding import PartitionSpec as P
import numpy as np

HEAD = 128
THETA = 10000
MESH = pl.DeviceIdType.MESH
F32, BF = jnp.float32, jnp.bfloat16

X0, F0, XD, YD, Y0, G0, HD, LD, ND, HI = 0, 2, 4, 5, 6, 8, 10, 11, 12, 13
N_REMOTE = 15
L_X, L_DY, L_G, L_COS, L_SIN, L_WQ, L_WK, L_WV, L_WO, L_AN, L_A0, L_YN, L_Y0, L_O, L_DQ, L_DKV, L_LO, L_NEAR = 0, 1, 2, 3, 4, 5, 6, 7, 8, 9, 10, 14, 15, 16, 17, 18, 19, 20
N_LOCAL = 22


def tables(rows):
    half = HEAD // 2
    rate = np.float32(THETA) ** (-np.arange(half, dtype=np.float32) / np.float32(half))
    angle = np.arange(rows, dtype=np.float32)[:, None] * rate.astype(np.float32)
    cos, sin = np.cos(angle).astype(np.float32), np.sin(angle).astype(np.float32)
    return np.concatenate([cos, cos], 1), np.concatenate([-sin, sin], 1)


def main_kernel(x_hbm, dy_hbm, gain_hbm, cos_hbm, sin_hbm, wq_hbm, wk_hbm, wv_hbm, wo_hbm,
                a_out, dy_out, o_out, dq_out, dkv_out, near_out, hi_out, lo_out,
                a_s, dy_s, gain_s, cos_s, sin_s, wq_s, wkv_s, wo_s, q_s, k_s, v_s, o_s, do_s, dq_s, dk32, dv32, dkv_s, lse_s, delta_s, top_s, mix_s,
                hi_recv, lo_recv, near_recv, near_stage, loc, snd, rcv):
    t = lax.axis_index("tp")
    chip, c = lax.div(t, 2), lax.rem(t, 2)
    partner, across = chip * 2 + 1 - c, (1 - chip) * 2 + c
    d = a_s.shape[1]
    half = d // 2
    R = x_hbm.shape[0]
    Q = R // 2
    heads = wq_hbm.shape[1] // HEAD
    cols = heads * R
    wide = 2 * R
    scale = HEAD**-0.5
    e = scale * LOG2E
    al = pl.multiple_of

    def local(src, dst, i):
        copy = pltpu.make_async_copy(src, dst, loc.at[i])
        copy.start()
        return copy

    def remote(src, dst, i, device, start=True):
        copy = pltpu.make_async_remote_copy(src_ref=src, dst_ref=dst, send_sem=snd.at[i], recv_sem=rcv.at[i], device_id={"tp": device}, device_id_type=MESH)
        if start:
            copy.start()
        return copy

    own = pl.ds(al(c * R, R), R)
    theirs = pl.ds(al((1 - c) * R, R), R)
    c_x = local(x_hbm, a_s.at[own], L_X)
    c_dy = local(dy_hbm, dy_s.at[own], L_DY)
    c_g = local(gain_hbm, gain_s, L_G)

    barrier = pltpu.get_barrier_semaphore()
    for k in range(1, 4):
        pl.semaphore_signal(barrier, inc=1, device_id={"tp": lax.rem(t + k, 4)}, device_id_type=MESH)
    pl.semaphore_wait(barrier, 3)

    def x_at(i, k):
        return pl.ds(al(2 * R + i * R + k * Q, Q), Q)

    sends = []
    x_ici = [remote(x_hbm.at[pl.ds(i * Q, Q)], a_s.at[x_at(i, c)], X0 + i, across) for i in range(2)]
    x_d2d = remote(x_hbm, a_s.at[own], XD, partner)
    dy_d2d = remote(dy_hbm, dy_s.at[own], YD, partner)
    sends += [*x_ici, x_d2d, dy_d2d]
    c_cos, c_sin = local(cos_hbm, cos_s, L_COS), local(sin_hbm, sin_s, L_SIN)
    c_wq = local(wq_hbm, wq_s, L_WQ)
    c_wk, c_wv = local(wk_hbm, wkv_s.at[:, pl.ds(0, HEAD)], L_WK), local(wv_hbm, wkv_s.at[:, pl.ds(HEAD, HEAD)], L_WV)
    c_wo = local(wo_hbm, wo_s, L_WO)

    def normed_rows(start, n):
        def body(i, _):
            r = pl.ds(al(start + i * 16, 16), 16)
            x = a_s[r, :].astype(F32)
            s = lax.rsqrt(jnp.mean(x * x, -1, keepdims=True) + 1e-6)
            a_s[r, :] = (x * s * gain_s[...].astype(F32)).astype(BF)

        lax.fori_loop(0, n // 16, body, None)

    def turn(ref, col, n_heads, start, n, sign):
        def body(i, _):
            r = pl.ds(al(start + i * 64, 64), 64)
            cs, sn = cos_s[r, :], sin_s[r, :]
            for h in range(n_heads):
                at = slice(col + h * HEAD, col + (h + 1) * HEAD)
                v = ref[r, at].astype(F32)
                ref[r, at] = (v * cs + sign * (pltpu.roll(v, HEAD // 2, 1) * sn)).astype(BF)

        lax.fori_loop(0, n // 64, body, None)

    near0, far0 = chip * 2 * R, (1 - chip) * 2 * R

    def project(src, places, n):
        r = _dot(a_s[src, :], wq_s[...], 1, 0).astype(BF)
        for i, p in enumerate(places):
            q_s[pl.ds(al(p, n), n), :] = r[i * n : (i + 1) * n]
        kv = _dot(a_s[src, :], wkv_s[...], 1, 0).astype(BF)
        for i, p in enumerate(places):
            k_s[pl.ds(al(p, n), n), :] = kv[i * n : (i + 1) * n, :HEAD]
            v_s[pl.ds(al(p, n), n), :] = kv[i * n : (i + 1) * n, HEAD:]
        for p in places:
            turn(q_s, 0, heads, p, n, 1.0)
            turn(k_s, 0, 1, p, n, 1.0)

    c_dy.wait()
    remote(dy_hbm, dy_s.at[theirs], YD, partner, False).wait_recv()

    def y_near(i):
        return pl.ds(al((1 - i) * R + c * Q, Q), Q)

    def y_far(i, k):
        return pl.ds(al(2 * R + (1 - i) * R + k * Q, Q), Q)

    dy_ici = [remote(dy_s.at[y_near(i)], dy_s.at[y_far(i, c)], Y0 + i, across) for i in range(2)]
    sends += dy_ici
    c_g.wait()
    c_x.wait()
    normed_rows(c * R, R)
    remote(x_hbm, a_s.at[theirs], XD, partner, False).wait_recv()
    normed_rows((1 - c) * R, R)
    c_an = local(a_s.at[pl.ds(0, 2 * R)], a_out.at[pl.ds(al(near0, 2 * R), 2 * R)], L_AN)
    for w in (c_cos, c_sin, c_wq, c_wk, c_wv):
        w.wait()
    project(pl.ds(0, 2 * R), [near0], 2 * R)
    c_wo.wait()
    c_yn = local(dy_s.at[pl.ds(0, 2 * R)], dy_out.at[pl.ds(al(near0, 2 * R), 2 * R)], L_YN)
    do_s[pl.ds(al(near0, 2 * R), 2 * R), :] = _dot(dy_s[pl.ds(0, 2 * R), :], wo_s[...], 1, 1).astype(BF)

    dk32[...] = jnp.zeros_like(dk32)
    dv32[...] = jnp.zeros_like(dv32)

    a_copies = [c_an, c_yn]
    for i in range(2):
        x_ici[i].wait_recv()
        give = remote(a_s.at[x_at(i, c)], a_s.at[x_at(i, c)], F0 + i, partner)
        remote(a_s.at[x_at(i, 1 - c)], a_s.at[x_at(i, 1 - c)], F0 + i, partner, False).wait_recv()
        give.wait_send()
        normed_rows(2 * R + i * R, R)
        places = [far0 + i * Q, far0 + R + i * Q]
        for k in range(2):
            a_copies.append(local(a_s.at[x_at(i, k)], a_out.at[pl.ds(al(places[k], Q), Q)], L_A0 + 2 * i + k))
        project(pl.ds(2 * R + i * R, R), places, Q)

    def seen_mask():
        return lax.rem(lax.broadcasted_iota(jnp.int32, (R, wide), 1), R) >= lax.broadcasted_iota(jnp.int32, (R, wide), 0)

    strips = range(0, cols, wide)

    def strip(ref, rows, at):
        h = at // R
        return jnp.concatenate([ref[rows, (h + n) * HEAD : (h + n + 1) * HEAD] for n in range(wide // R)], axis=0)

    def attend_block(b, _):
        rows = pl.ds(al(b * R, R), R)
        top_s[...] = jnp.full(top_s.shape, NEG, F32)
        mix_s[...] = jnp.zeros_like(mix_s)

        def pair(j, masked):
            here = pl.ds(al(j * R, R), R)
            keys = k_s[here, :]
            values = jnp.concatenate([v_s[here, :].T, jnp.ones((8, R), BF)], axis=0)
            scores = [_dot(keys, strip(q_s, rows, at), 1, 1) for at in strips]
            weights, keeps = [], []
            for at, s in zip(strips, scores):
                if masked:
                    s = jnp.where(seen_mask(), s, HIDDEN)
                old = top_s[:, at : at + wide]
                top = jnp.maximum(old, s.max(axis=0, keepdims=True))
                top_s[:, at : at + wide] = top
                weights.append(jnp.exp2((s - top) * e).astype(BF))
                keeps.append(jnp.exp2((old - top) * e))
            for at, p, keep in zip(strips, weights, keeps):
                mix_s[:, at : at + wide] = mix_s[:, at : at + wide] * keep + _dot(values, p, 1, 0)

        lax.fori_loop(0, b, lambda j, _: pair(j, False), None)
        pair(b, True)
        total = mix_s[HEAD : HEAD + 1, :]
        out = (mix_s[:HEAD, :] * (1 / total)).T.astype(BF)
        for h in range(heads):
            o_s[rows, h * HEAD : (h + 1) * HEAD] = out[h * R : (h + 1) * R]
        lse_s[b] = top_s[...] * scale + jnp.log(total)

    lax.fori_loop(0, 4, attend_block, None)
    c_o = local(o_s, o_out, L_O)

    def backward_block(b):
        rows = pl.ds(al(b * R, R), R)
        for at in strips:
            both = strip(do_s, rows, at).astype(F32) * strip(o_s, rows, at).astype(F32)
            delta_s[:, at : at + wide] = both.T.sum(axis=0, keepdims=True)
        mix_s[...] = jnp.zeros_like(mix_s)

        def pair(j, masked):
            here = pl.ds(al(j * R, R), R)
            keys, values = k_s[here, :], v_s[here, :]
            keys_t = keys.T
            dv = dk = None
            for at in strips:
                q, do = strip(q_s, rows, at), strip(do_s, rows, at)
                p = jnp.exp2(_dot(keys, q, 1, 1) * e - lse_s[b, :, at : at + wide] * LOG2E)
                if masked:
                    p = jnp.where(seen_mask(), p, 0.0)
                ds = (p * (_dot(values, do, 1, 1) - delta_s[:, at : at + wide])).astype(BF)
                a, g = _dot(p.astype(BF), do, 1, 0), _dot(ds, q, 1, 0)
                dv, dk = (a, g) if dv is None else (dv + a, dk + g)
                mix_s[:HEAD, at : at + wide] += _dot(keys_t, ds, 1, 0)
            dv32[here, :] += dv
            dk32[here, :] += dk

        lax.fori_loop(0, b, lambda j, _: pair(j, False), None)
        pair(b, True)
        out = (mix_s[:HEAD, :] * scale).T
        cs, sn = cos_s[rows, :], sin_s[rows, :]
        for h in range(heads):
            g = out[h * R : (h + 1) * R]
            dq_s[rows, h * HEAD : (h + 1) * HEAD] = (g * cs - pltpu.roll(g, HEAD // 2, 1) * sn).astype(BF)

    def keys_done(b):
        rows = pl.ds(al(b * R, R), R)
        g = dk32[rows, :] * scale
        dkv_s[rows, :HEAD] = (g * cos_s[rows, :] - pltpu.roll(g, HEAD // 2, 1) * sin_s[rows, :]).astype(BF)
        dkv_s[rows, HEAD:] = dv32[rows, :].astype(BF)

    def term(b, k):
        rows, at = pl.ds(al(b * R, R), R), pl.ds(al(k * half, half), half)
        return _dot(dq_s[rows, :], wq_s[at, :], 1, 1) + _dot(dkv_s[rows, :], wkv_s[at, :], 1, 1)

    near_hi, near_lo = chip * 2 + 1, chip * 2
    far_hi, far_lo = (1 - chip) * 2 + 1, (1 - chip) * 2

    def pass_on(i):
        dy_ici[i].wait_recv()
        return remote(dy_s.at[y_far(i, c)], dy_s.at[y_far(i, c)], G0 + i, partner)

    backward_block(near_hi)
    sends.append(pass_on(0))
    backward_block(near_lo)
    for copy in a_copies:
        copy.wait()
    last = []
    c_lo = None
    for i, b in ((0, far_hi), (1, far_lo)):
        if i == 1:
            sends.append(pass_on(1))
        remote(dy_s.at[y_far(i, 1 - c)], dy_s.at[y_far(i, 1 - c)], G0 + i, partner, False).wait_recv()
        block = pl.ds(2 * R + (1 - i) * R, R)
        last.append(local(dy_s.at[block], dy_out.at[pl.ds(al(b * R, R), R)], L_Y0 if i == 0 else L_YN))
        do_s[pl.ds(al(b * R, R), R), :] = _dot(dy_s[block, :], wo_s[...], 1, 1).astype(BF)
        backward_block(b)
        keys_done(b)
        out, total, got = a_s.at[pl.ds(2 * i * R, R), pl.ds(0, half)], a_s.at[pl.ds(2 * i * R, R), pl.ds(half, half)], (hi_recv, lo_recv)[i]
        out[...] = term(b, 1 - c).astype(BF)
        swap = remote(out, got, HD + i, partner)
        sends.append(swap)
        mine = term(b, c)
        swap.wait_recv()
        total[...] = (mine + got[...].astype(F32)).astype(BF)
        if i == 0:
            sends.append(pltpu.make_async_remote_copy(src_ref=total, dst_ref=hi_out.at[c], send_sem=snd.at[HI], recv_sem=rcv.at[HI + c], device_id={"tp": (1 - chip) * 2 + 1}, device_id_type=MESH))
            sends[-1].start()
        else:
            last.append(local(total, lo_out, L_LO))
    last.append(local(dq_s, dq_out, L_DQ))
    keys_done(near_hi)
    keys_done(near_lo)
    last.append(local(dkv_s, dkv_out, L_DKV))
    for k in range(2):
        a_s[pl.ds(R, R), k * half : (k + 1) * half] = term(chip * 2 + 1 - c, k).astype(BF)
    swap = remote(a_s.at[pl.ds(R, R)], near_recv, ND, partner)
    sends.append(swap)
    for k in range(2):
        mine = term(chip * 2 + c, k)
        if k == 0:
            swap.wait_recv()
        else:
            last[-1].wait()
            last.pop()
        near_stage[...] = mine + near_recv[:, k * half : (k + 1) * half].astype(F32)
        last.append(local(near_stage, near_out.at[:, pl.ds(k * half, half)], L_NEAR + k))

    @pl.when(c == 1)
    def _():
        for k in range(2):
            pltpu.make_async_remote_copy(src_ref=hi_out.at[k], dst_ref=hi_out.at[k], send_sem=snd.at[HI], recv_sem=rcv.at[HI + k], device_id={"tp": across}, device_id_type=MESH).wait_recv()

    for copy in sends:
        copy.wait_send()
    c_o.wait()
    for copy in last:
        copy.wait()


def main(x, dy, gain, wq, wk, wv, wo):
    R, d = x.shape
    n, width = 4 * R, wq.shape[1]
    heads = width // HEAD
    cos, sin = tables(n)
    any_ = pl.BlockSpec(memory_space=pl.ANY)
    vm = pltpu.VMEM
    flops = 2 * n * d * (3 * width + 4 * HEAD) + 7 * n * n * width
    return pl.pallas_call(
        main_kernel,
        in_specs=[any_] * 9,
        out_specs=[any_] * 8,
        out_shape=[jax.ShapeDtypeStruct((n, d), BF), jax.ShapeDtypeStruct((n, d), BF), jax.ShapeDtypeStruct((n, width), BF), jax.ShapeDtypeStruct((n, width), BF),
                   jax.ShapeDtypeStruct((n, 2 * HEAD), BF), jax.ShapeDtypeStruct((R, d), F32), jax.ShapeDtypeStruct((2, R, d // 2), BF), jax.ShapeDtypeStruct((R, d // 2), BF)],
        scratch_shapes=[vm((n, d), BF), vm((n, d), BF), vm((1, d), BF), vm((n, HEAD), F32), vm((n, HEAD), F32), vm((d, width), BF), vm((d, 2 * HEAD), BF), vm((width, d), BF),
                        vm((n, width), BF), vm((n, HEAD), BF), vm((n, HEAD), BF), vm((n, width), BF), vm((n, width), BF), vm((n, width), BF),
                        vm((n, HEAD), F32), vm((n, HEAD), F32), vm((n, 2 * HEAD), BF), vm((4, 1, heads * R), F32), vm((1, heads * R), F32), vm((1, heads * R), F32), vm((HEAD + 8, heads * R), F32),
                        vm((R, d // 2), BF), vm((R, d // 2), BF), vm((R, d), BF), vm((R, d // 2), F32),
                        pltpu.SemaphoreType.DMA((N_LOCAL,)), pltpu.SemaphoreType.DMA((N_REMOTE,)), pltpu.SemaphoreType.DMA((N_REMOTE,))],
        compiler_params=pltpu.CompilerParams(collective_id=0, has_side_effects=True, vmem_limit_bytes=67043328),
        cost_estimate=pl.CostEstimate(flops=flops, bytes_accessed=60 * 2**20, transcendentals=n * n * heads),
        name="main",
    )(x, dy, gain.reshape(1, d), jnp.asarray(cos), jnp.asarray(sin), wq, wk, wv, wo)


def weights_kernel(a_ref, dq_ref, dkv_ref, o_ref, dy_ref, wq_ref, wk_ref, wv_ref, wo_ref):
    a = a_ref[...]
    wq_ref[...] = _dot(a, dq_ref[...], 0, 0).astype(BF)
    kv = _dot(a, dkv_ref[...], 0, 0).astype(BF)
    wk_ref[...] = kv[:, :HEAD]
    wv_ref[...] = kv[:, HEAD:]
    wo_ref[...] = _dot(o_ref[...], dy_ref[...], 0, 0).astype(BF)


def weight_gradients(a, dq, dkv, o, dy, tile=512):
    n, d = a.shape
    width = dq.shape[1]
    tall = pl.BlockSpec((n, tile), lambda i: (0, i))
    whole = lambda w: pl.BlockSpec((n, w), lambda i: (0, 0))
    rows = lambda w: pl.BlockSpec((tile, w), lambda i: (i, 0))
    return pl.pallas_call(
        weights_kernel,
        grid=(d // tile,),
        in_specs=[tall, whole(width), whole(2 * HEAD), whole(width), tall],
        out_specs=[rows(width), rows(HEAD), rows(HEAD), pl.BlockSpec((width, tile), lambda i: (0, i))],
        out_shape=[jax.ShapeDtypeStruct((d, width), BF), jax.ShapeDtypeStruct((d, HEAD), BF), jax.ShapeDtypeStruct((d, HEAD), BF), jax.ShapeDtypeStruct((width, d), BF)],
        compiler_params=pltpu.CompilerParams(dimension_semantics=("arbitrary",), vmem_limit_bytes=VMEM),
        cost_estimate=pl.CostEstimate(flops=2 * n * d * (2 * width + 2 * HEAD), bytes_accessed=2 * (2 * n * d + 2 * n * width + 2 * d * width), transcendentals=0),
        name="weights",
    )(a, dq, dkv, o, dy)


def solution(mesh):
    def step(x, dy, gain, wq, wk, wv, wo):
        a, dy_all, o, dq, dkv, near, hi, lo = main(x, dy, gain, wq, wk, wv, wo)
        lo0 = lax.ppermute(lo, "tp", [(0, 2), (2, 0)])
        lo1 = lax.ppermute(lo, "tp", [(1, 2), (3, 0)])
        by_wq, by_wk, by_wv, by_wo = weight_gradients(a, dq, dkv, o, dy_all)
        upper = lax.rem(lax.axis_index("tp"), 2) == 1
        far = jnp.concatenate([jnp.where(upper, hi[0], lo0), jnp.where(upper, hi[1], lo1)], 1)
        da = near + far.astype(F32)
        wide = x.astype(F32)
        s = lax.rsqrt(jnp.mean(wide * wide, -1, keepdims=True) + 1e-6)
        g = da * gain.astype(F32)
        by_gain = jnp.sum(da * (wide * s), 0, keepdims=True)
        by_x = (dy.astype(F32) + s * g - wide * (s * s * s) * jnp.mean(g * wide, -1, keepdims=True)).astype(BF)
        by_gain = by_gain + lax.ppermute(by_gain, "tp", [(0, 1), (1, 0), (2, 3), (3, 2)])
        by_gain = by_gain + lax.ppermute(by_gain, "tp", [(0, 2), (2, 0), (1, 3), (3, 1)])
        return by_x, by_gain, by_wq, by_wk, by_wv, by_wo

    tokens, columns = P(("dp", "tp"), None), P(None, "tp")
    return jax.shard_map(
        step,
        mesh=mesh,
        in_specs=(tokens, tokens, P(None), columns, columns, columns, P("tp", None)),
        out_specs=(tokens, P("dp", None), P("dp", "tp"), P("dp", "tp"), P("dp", "tp"), P(("dp", "tp"), None)),
        check_vma=False,
    )
```

```python
import functools

import jax
import jax.numpy as jnp
from jax import lax
from jax.experimental import pallas as pl
from jax.experimental.pallas import tpu as pltpu

NEG = -1e30
HIDDEN = 2 * NEG
LOG2E = 1.4426950408889634
VMEM = 56 * 2**20


def _dot(a, b, ca, cb):
    return lax.dot_general(a, b, (((ca,), (cb,)), ((), ())), preferred_element_type=jnp.float32)


from jax.sharding import PartitionSpec as P
import numpy as np

HEAD = 128
THETA = 10000
MESH = pl.DeviceIdType.MESH
F32, BF = jnp.float32, jnp.bfloat16

X0, F0, XD, YD, Y0, G0, HD, LD, ND, HI = 0, 2, 4, 5, 6, 8, 10, 11, 13, 15
N_REMOTE = 17
L_X, L_DY, L_G, L_COS, L_WQ, L_WK, L_WV, L_WO, L_YN, L_A0, L_Y0, L_O, L_DQ, L_DKV, L_LO, L_NEAR = 0, 1, 2, 3, 4, 5, 6, 7, 8, 9, 17, 19, 20, 21, 22, 24
N_LOCAL = 26
FINE = 32


def tables(rows):
    half = HEAD // 2
    rate = float(THETA) ** (-np.arange(half, dtype=np.float64) / half)
    place = np.concatenate([np.arange(0, rows, FINE), np.arange(FINE)]).astype(np.float64)
    angle = place[:, None] * np.concatenate([rate, rate])[None]
    return np.cos(angle).astype(np.float32), np.sin(angle).astype(np.float32)


def main_kernel(x_hbm, dy_hbm, gain_hbm, table_hbm, wq_hbm, wk_hbm, wv_hbm, wo_hbm,
                a_out, dy_out, o_out, dq_out, dkv_out, near_out, hi_out, lo_out, gain_out,
                a_s, dy_s, gain_1, gain_s, table_s, cos_s, sin_s, wq_s, wkv_s, wo_s, q_s, k_s, v_s, o_s, do_s, dq_s, dk32, dv32, dkv_s, lse_s, delta_s, top_s, mix_s,
                recv_s, near_recv, stage, loc, snd, rcv):
    t = lax.axis_index("tp")
    chip, c = lax.div(t, 2), lax.rem(t, 2)
    partner, across = chip * 2 + 1 - c, (1 - chip) * 2 + c
    d = a_s.shape[1]
    half = d // 2
    R = x_hbm.shape[0]
    Q = R // 2
    heads = wq_hbm.shape[1] // HEAD
    cols = heads * R
    wide = 2 * R
    scale = HEAD**-0.5
    e = scale * LOG2E
    al = pl.multiple_of

    def local(src, dst, i):
        copy = pltpu.make_async_copy(src, dst, loc.at[i])
        copy.start()
        return copy

    def remote(src, dst, i, device, start=True):
        copy = pltpu.make_async_remote_copy(src_ref=src, dst_ref=dst, send_sem=snd.at[i], recv_sem=rcv.at[i], device_id={"tp": device}, device_id_type=MESH)
        if start:
            copy.start()
        return copy

    own = pl.ds(al(c * R, R), R)
    theirs = pl.ds(al((1 - c) * R, R), R)
    c_x = local(x_hbm, a_s.at[own], L_X)
    c_dy = local(dy_hbm, dy_s.at[own], L_DY)
    c_g = local(gain_hbm, gain_1, L_G)

    barrier = pltpu.get_barrier_semaphore()
    for k in range(1, 4):
        pl.semaphore_signal(barrier, inc=1, device_id={"tp": lax.rem(t + k, 4)}, device_id_type=MESH)
    pl.semaphore_wait(barrier, 3)

    def x_at(i, k):
        return pl.ds(al(2 * R + i * R + k * Q, Q), Q)

    def y_near(i):
        return pl.ds(al((1 - i) * R + c * Q, Q), Q)

    def y_far(i, k):
        return pl.ds(al(2 * R + (1 - i) * R + k * Q, Q), Q)

    sends = []
    sends += [remote(x_hbm.at[pl.ds(i * Q, Q)], near_recv.at[pl.ds(i * Q, Q)], X0 + i, across) for i in range(2)]
    sends += [remote(x_hbm, a_s.at[own], XD, partner), remote(dy_hbm, dy_s.at[own], YD, partner)]
    c_table = local(table_hbm, table_s, L_COS)
    c_wq = local(wq_hbm, wq_s, L_WQ)
    c_wk, c_wv = local(wk_hbm, wkv_s.at[:, pl.ds(0, HEAD)], L_WK), local(wv_hbm, wkv_s.at[:, pl.ds(HEAD, HEAD)], L_WV)
    c_wo = local(wo_hbm, wo_s, L_WO)

    def normed_rows(src, first, start, n):
        def body(i, _):
            x = src[pl.ds(al(first + i * 16, 16), 16), :].astype(F32)
            s = lax.rsqrt(jnp.mean(x * x, -1, keepdims=True) + 1e-6)
            a_s[pl.ds(al(start + i * 16, 16), 16), :] = (x * s * gain_s[...]).astype(BF)

        lax.fori_loop(0, n // 16, body, None)

    def turn(ref, n_heads, start, n):
        def body(i, _):
            r = pl.ds(al(start + i * 32, 32), 32)
            cs, sn = cos_s[r, :], sin_s[r, :]
            for h in range(n_heads):
                at = slice(h * HEAD, (h + 1) * HEAD)
                v = ref[r, at].astype(F32)
                ref[r, at] = (v * cs + pltpu.roll(v, HEAD // 2, 1) * sn).astype(BF)

        lax.fori_loop(0, n // 32, body, None)

    near0, far0 = chip * 2 * R, (1 - chip) * 2 * R

    c_dy.wait()
    remote(dy_hbm, dy_s.at[theirs], YD, partner, False).wait_recv()
    dy_ici = [remote(dy_s.at[y_near(i)], dy_s.at[y_far(i, c)], Y0 + i, across) for i in range(2)]
    sends += dy_ici
    c_g.wait()
    gain_s[...] = gain_1[...].astype(F32).reshape(1, d)
    c_table.wait()
    c_gain = local(gain_s, gain_out, L_G)
    few = cos_s.shape[0] // FINE
    side = jnp.where(lax.broadcasted_iota(jnp.int32, (1, HEAD), 1) < HEAD // 2, -1.0, 1.0)

    def angles(i, _):
        r = pl.ds(al(i * FINE, FINE), FINE)
        ca, sa = table_s[0, pl.ds(i, 1), :], table_s[1, pl.ds(i, 1), :]
        cb, sb = table_s[0, few:, :], table_s[1, few:, :]
        cos_s[r, :] = ca * cb - sa * sb
        sin_s[r, :] = (sa * cb + ca * sb) * side

    lax.fori_loop(0, few, angles, None)
    c_x.wait()
    remote(x_hbm, a_s.at[theirs], XD, partner, False).wait_recv()

    def a_copy(i, k):
        token = jnp.where(i < 2, near0 + i * R + k * Q, far0 + (i - 2) * Q + k * R)
        return pltpu.make_async_copy(a_s.at[pl.ds(al(i * R + k * Q, Q), Q)], a_out.at[pl.ds(al(token, Q), Q)], loc.at[L_A0 + 2 * i + k])

    def project_block(i, _):
        @pl.when(i >= 2)
        def _():
            j = i - 2
            landed = near_recv.at[pl.ds(al(j * Q, Q), Q)]
            remote(x_hbm.at[pl.ds(0, Q)], landed, X0 + j, across, False).wait_recv()
            give = remote(landed, a_s.at[x_at(j, c)], F0 + j, partner)
            normed_rows(near_recv, j * Q, 2 * R + j * R + c * Q, Q)
            remote(landed, a_s.at[x_at(j, 1 - c)], F0 + j, partner, False).wait_recv()
            normed_rows(a_s, 2 * R + j * R + (1 - c) * Q, 2 * R + j * R + (1 - c) * Q, Q)
            give.wait_send()

        @pl.when(i < 2)
        def _():
            normed_rows(a_s, i * R, i * R, R)

        for k in range(2):
            a_copy(i, k).start()

        @pl.when(i == 0)
        def _():
            for w in (c_wq, c_wk, c_wv):
                w.wait()

        block = pl.ds(al(i * R, R), R)
        r = _dot(a_s[block, :], wq_s[...], 1, 0).astype(BF)
        kv = _dot(a_s[block, :], wkv_s[...], 1, 0).astype(BF)
        for k in range(2):
            token = jnp.where(i < 2, near0 + i * R + k * Q, far0 + (i - 2) * Q + k * R)
            p = pl.ds(al(token, Q), Q)
            q_s[p, :] = r[k * Q : (k + 1) * Q]
            k_s[p, :] = kv[k * Q : (k + 1) * Q, :HEAD]
            v_s[p, :] = kv[k * Q : (k + 1) * Q, HEAD:]
            turn(q_s, heads, token, Q)
            turn(k_s, 1, token, Q)

        @pl.when(i < 2)
        def _():
            @pl.when(i == 0)
            def _():
                c_wo.wait()

            do_s[pl.ds(al(near0 + i * R, R), R), :] = _dot(dy_s[block, :], wo_s[...], 1, 1).astype(BF)

    dk32[...] = jnp.zeros_like(dk32)
    dv32[...] = jnp.zeros_like(dv32)
    lax.fori_loop(0, 4, project_block, None)
    c_yn = local(dy_s.at[pl.ds(0, 2 * R)], dy_out.at[pl.ds(al(near0, 2 * R), 2 * R)], L_YN)

    def seen_mask():
        return lax.rem(lax.broadcasted_iota(jnp.int32, (R, wide), 1), R) >= lax.broadcasted_iota(jnp.int32, (R, wide), 0)

    strips = range(0, cols, wide)

    def strip(ref, rows, at):
        h = at // R
        return jnp.concatenate([ref[rows, (h + n) * HEAD : (h + n + 1) * HEAD] for n in range(wide // R)], axis=0)

    def attend_block(b, _):
        rows = pl.ds(al(b * R, R), R)
        top_s[...] = jnp.full(top_s.shape, NEG, F32)
        mix_s[...] = jnp.zeros_like(mix_s)

        def pair(j, masked):
            here = pl.ds(al(j * R, R), R)
            keys = k_s[here, :]
            values = jnp.concatenate([v_s[here, :].T, jnp.ones((8, R), BF)], axis=0)
            scores = [_dot(keys, strip(q_s, rows, at), 1, 1) for at in strips]
            weights, keeps = [], []
            for at, s in zip(strips, scores):
                if masked:
                    s = jnp.where(seen_mask(), s, HIDDEN)
                old = top_s[:, at : at + wide]
                top = jnp.maximum(old, s.max(axis=0, keepdims=True))
                top_s[:, at : at + wide] = top
                weights.append(jnp.exp2((s - top) * e).astype(BF))
                keeps.append(jnp.exp2((old - top) * e))
            for at, p, keep in zip(strips, weights, keeps):
                mix_s[:, at : at + wide] = mix_s[:, at : at + wide] * keep + _dot(values, p, 1, 0)

        lax.fori_loop(0, b, lambda j, _: pair(j, False), None)
        pair(b, True)
        total = mix_s[HEAD : HEAD + 1, :]
        out = (mix_s[:HEAD, :] * (1 / total)).T.astype(BF)
        for h in range(heads):
            o_s[rows, h * HEAD : (h + 1) * HEAD] = out[h * R : (h + 1) * R]
        lse_s[b] = top_s[...] * scale + jnp.log(total)

    lax.fori_loop(0, 4, attend_block, None)
    c_o = local(o_s, o_out, L_O)

    def backward_block(b):
        rows = pl.ds(al(b * R, R), R)
        for at in strips:
            both = strip(do_s, rows, at).astype(F32) * strip(o_s, rows, at).astype(F32)
            delta_s[:, at : at + wide] = both.T.sum(axis=0, keepdims=True)
        mix_s[...] = jnp.zeros_like(mix_s)

        def pair(j, masked):
            here = pl.ds(al(j * R, R), R)
            keys, values = k_s[here, :], v_s[here, :]
            keys_t = keys.T
            dv = dk = None
            for at in strips:
                q, do = strip(q_s, rows, at), strip(do_s, rows, at)
                p = jnp.exp2(_dot(keys, q, 1, 1) * e - lse_s[b, :, at : at + wide] * LOG2E)
                if masked:
                    p = jnp.where(seen_mask(), p, 0.0)
                ds = (p * (_dot(values, do, 1, 1) - delta_s[:, at : at + wide])).astype(BF)
                a, g = _dot(p.astype(BF), do, 1, 0), _dot(ds, q, 1, 0)
                dv, dk = (a, g) if dv is None else (dv + a, dk + g)
                mix_s[:HEAD, at : at + wide] += _dot(keys_t, ds, 1, 0)
            dv32[here, :] += dv
            dk32[here, :] += dk

        lax.fori_loop(0, b, lambda j, _: pair(j, False), None)
        pair(b, True)
        out = (mix_s[:HEAD, :] * scale).T
        cs, sn = cos_s[rows, :], sin_s[rows, :]
        for h in range(heads):
            g = out[h * R : (h + 1) * R]
            dq_s[rows, h * HEAD : (h + 1) * HEAD] = (g * cs - pltpu.roll(g, HEAD // 2, 1) * sn).astype(BF)

    def keys_done(b):
        rows = pl.ds(al(b * R, R), R)
        g = dk32[rows, :] * scale
        dkv_s[rows, :HEAD] = (g * cos_s[rows, :] - pltpu.roll(g, HEAD // 2, 1) * sin_s[rows, :]).astype(BF)
        dkv_s[rows, HEAD:] = dv32[rows, :].astype(BF)

    def term(b, k):
        rows, at = pl.ds(al(b * R, R), R), pl.ds(al(k * half, half), half)
        return _dot(dq_s[rows, :], wq_s[at, :], 1, 1) + _dot(dkv_s[rows, :], wkv_s[at, :], 1, 1)

    def dy_copy(i, b):
        return pltpu.make_async_copy(dy_s.at[pl.ds(al(2 * R + (1 - i) * R, R), R)], dy_out.at[pl.ds(al(b * R, R), R)], loc.at[L_Y0 + i])

    swap_hi = remote(a_s.at[pl.ds(0, R), pl.ds(0, half)], recv_s.at[0], HD, partner, False)

    def hi_copy(k):
        return pltpu.make_async_remote_copy(src_ref=a_s.at[pl.ds(0, R), pl.ds(half, half)], dst_ref=hi_out.at[k], send_sem=snd.at[HI], recv_sem=rcv.at[HI + k],
                                            device_id={"tp": (1 - chip) * 2 + 1}, device_id_type=MESH)

    def backward_step(s, _):
        i = s - 2
        b = jnp.where(s < 2, chip * 2 + 1 - s, (1 - chip) * 2 + 1 - i)

        @pl.when((s == 1) | (s == 3))
        def _():
            j = lax.div(s, 2)
            remote(dy_s.at[y_near(0)], dy_s.at[y_far(j, c)], Y0 + j, across, False).wait_recv()
            remote(dy_s.at[y_far(j, c)], dy_s.at[y_far(j, c)], G0 + j, partner)

        @pl.when(s == 2)
        def _():
            for k in range(4):
                for n in range(2):
                    a_copy(k, n).wait()

        @pl.when(s >= 2)
        def _():
            remote(dy_s.at[y_far(i, 1 - c)], dy_s.at[y_far(i, 1 - c)], G0 + i, partner, False).wait_recv()
            dy_copy(i, b).start()
            do_s[pl.ds(al(b * R, R), R), :] = _dot(dy_s[pl.ds(al(2 * R + (1 - i) * R, R), R), :], wo_s[...], 1, 1).astype(BF)

        backward_block(b)

        @pl.when(s >= 2)
        def _():
            keys_done(b)

            @pl.when(i == 0)
            def _():
                a_s[:R, :half] = term(b, 1 - c).astype(BF)
                swap_hi.start()
                mine = term(b, c)
                swap_hi.wait_recv()
                a_s[:R, half:] = (mine + recv_s[0].astype(F32)).astype(BF)
                hi_copy(c).start()

    lax.fori_loop(0, 4, backward_step, None)
    c_dq = local(dq_s, dq_out, L_DQ)
    keys_done(chip * 2)
    keys_done(chip * 2 + 1)
    c_dkv = local(dkv_s, dkv_out, L_DKV)

    def place(i, k):
        return pl.ds(al(R + i * R, R), R), pl.ds(al(k * half, half), half)

    def give_half(i, k):
        rows, at = place(i, k)
        return remote(a_s.at[rows, at], near_recv.at[:, at] if i == 0 else recv_s.at[k], (ND if i == 0 else LD) + k, partner, False)

    def lo_copy(k):
        rows, at = place(1, k)
        return pltpu.make_async_copy(a_s.at[rows, at], lo_out.at[:, at], loc.at[L_LO + k])

    def near_copy(k):
        return pltpu.make_async_copy(stage.at[k], near_out.at[:, pl.ds(al(k * half, half), half)], loc.at[L_NEAR + k])

    def give_part(n, _):
        k, low = lax.rem(n, 2), lax.div(n, 2) != c
        b = jnp.where(low, (1 - chip) * 2, chip * 2 + 1 - c)

        @pl.when(low & (c == 0))
        def _():
            rows, at = place(1, k)
            mine = term(b, k)
            give_half(1, k).wait_recv()
            a_s[rows, at] = (mine + recv_s[k].astype(F32)).astype(BF)
            lo_copy(k).start()

        @pl.when(jnp.logical_not(low & (c == 0)))
        def _():
            rows, at = place(jnp.where(low, 1, 0), k)
            a_s[rows, at] = term(b, k).astype(BF)

            @pl.when(low)
            def _():
                give_half(1, k).start()

            @pl.when(jnp.logical_not(low))
            def _():
                give_half(0, k).start()

    lax.fori_loop(0, 4, give_part, None)

    def own_part(k, _):
        mine = term(chip * 2 + c, k)
        give_half(0, k).wait_recv()
        stage[k] = mine + near_recv[:, pl.ds(al(k * half, half), half)].astype(F32)
        near_copy(k).start()

    lax.fori_loop(0, 2, own_part, None)

    @pl.when(c == 1)
    def _():
        for k in range(2):
            hi_copy(k).wait_recv()

    @pl.when(c == 0)
    def _():
        for k in range(2):
            lo_copy(k).wait()

    @pl.when(c == 1)
    def _():
        for k in range(2):
            give_half(1, k).wait_send()

    for i in range(2):
        remote(dy_s.at[y_far(i, c)], dy_s.at[y_far(i, c)], G0 + i, partner, False).wait_send()
        dy_copy(i, (1 - chip) * 2 + 1 - i).wait()
        give_half(0, i).wait_send()
        near_copy(i).wait()
    for copy in (*sends, swap_hi, hi_copy(c)):
        copy.wait_send()
    for copy in (c_gain, c_o, c_yn, c_dq, c_dkv):
        copy.wait()


def main(x, dy, gain, wq, wk, wv, wo):
    R, d = x.shape
    n, width = 4 * R, wq.shape[1]
    heads = width // HEAD
    table = jnp.asarray(np.stack(tables(n)))
    any_ = pl.BlockSpec(memory_space=pl.ANY)
    vm = pltpu.VMEM
    flops = 2 * n * d * (3 * width + 4 * HEAD) + 7 * n * n * width
    return pl.pallas_call(
        main_kernel,
        in_specs=[any_] * 8,
        out_specs=[any_] * 9,
        out_shape=[jax.ShapeDtypeStruct((n, d), BF), jax.ShapeDtypeStruct((n, d), BF), jax.ShapeDtypeStruct((n, width), BF), jax.ShapeDtypeStruct((n, width), BF),
                   jax.ShapeDtypeStruct((n, 2 * HEAD), BF), jax.ShapeDtypeStruct((R, d), F32), jax.ShapeDtypeStruct((2, R, d // 2), BF), jax.ShapeDtypeStruct((R, d), BF), jax.ShapeDtypeStruct((1, d), F32)],
        scratch_shapes=[vm((n, d), BF), vm((n, d), BF), vm((d,), BF), vm((1, d), F32), vm(table.shape, F32), vm((n, HEAD), F32), vm((n, HEAD), F32), vm((d, width), BF), vm((d, 2 * HEAD), BF), vm((width, d), BF),
                        vm((n, width), BF), vm((n, HEAD), BF), vm((n, HEAD), BF), vm((n, width), BF), vm((n, width), BF), vm((n, width), BF),
                        vm((n, HEAD), F32), vm((n, HEAD), F32), vm((n, 2 * HEAD), BF), vm((4, 1, heads * R), F32), vm((1, heads * R), F32), vm((1, heads * R), F32), vm((HEAD + 8, heads * R), F32),
                        vm((2, R, d // 2), BF), vm((R, d), BF), vm((2, R, d // 2), F32),
                        pltpu.SemaphoreType.DMA((N_LOCAL,)), pltpu.SemaphoreType.DMA((N_REMOTE,)), pltpu.SemaphoreType.DMA((N_REMOTE,))],
        compiler_params=pltpu.CompilerParams(collective_id=0, has_side_effects=True, vmem_limit_bytes=67043328),
        cost_estimate=pl.CostEstimate(flops=flops, bytes_accessed=60 * 2**20, transcendentals=n * n * heads),
        name="main",
    )(x, dy, gain, table, wq, wk, wv, wo)


def row_scale(x):
    return lax.rsqrt(jnp.mean(x * x, -1, keepdims=True) + 1e-6)


def weights_kernel(a_ref, dq_ref, dkv_ref, o_ref, dy_ref, wq_ref, wk_ref, wv_ref, wo_ref):
    a = a_ref[...]
    wq_ref[...] = _dot(a, dq_ref[...], 0, 0).astype(BF)
    kv = _dot(a, dkv_ref[...], 0, 0).astype(BF)
    wk_ref[...] = kv[:, :HEAD]
    wv_ref[...] = kv[:, HEAD:]
    wo_ref[...] = _dot(o_ref[...], dy_ref[...], 0, 0).astype(BF)


def weight_gradients(a, dq, dkv, o, dy, tile=512):
    n, d = a.shape
    width = dq.shape[1]
    tall = pl.BlockSpec((n, tile), lambda i: (0, i))
    whole = lambda w: pl.BlockSpec((n, w), lambda i: (0, 0))
    rows = lambda w: pl.BlockSpec((tile, w), lambda i: (i, 0))
    return pl.pallas_call(
        weights_kernel,
        grid=(d // tile,),
        in_specs=[tall, whole(width), whole(2 * HEAD), whole(width), tall],
        out_specs=[rows(width), rows(HEAD), rows(HEAD), pl.BlockSpec((width, tile), lambda i: (0, i))],
        out_shape=[jax.ShapeDtypeStruct((d, width), BF), jax.ShapeDtypeStruct((d, HEAD), BF), jax.ShapeDtypeStruct((d, HEAD), BF), jax.ShapeDtypeStruct((width, d), BF)],
        compiler_params=pltpu.CompilerParams(dimension_semantics=("arbitrary",), vmem_limit_bytes=62 * 2**20),
        cost_estimate=pl.CostEstimate(flops=2 * n * d * (2 * width + 2 * HEAD), bytes_accessed=2 * (2 * n * d + 2 * n * width + 2 * d * width), transcendentals=0),
        name="weights",
    )(a, dq, dkv, o, dy)


def close_kernel(chunk, step, x_hbm, dy_hbm, near_hbm, hi_hbm, lo_hbm, gain_ref, dx_hbm, dgain_ref, x_s, dy_s, near_s, far_s, dx_s, sum_s, part_s, got_s, in_sem, out_sem, snd, rcv):
    R, d = x_s.shape
    half = d // 2
    t = lax.axis_index("tp")
    chip, c = lax.div(t, 2), lax.rem(t, 2)
    peers = [chip * 2 + 1 - c, (1 - chip) * 2 + c, (1 - chip) * 2 + 1 - c]
    upper = c == 1
    n = R // chunk

    def loads(i):
        r = pl.ds(i * chunk, chunk)
        return [pltpu.make_async_copy(src.at[r], dst.at[r], in_sem.at[i, k]) for k, (src, dst) in enumerate(((x_hbm, x_s), (near_hbm, near_s)))]

    def load_dy(i):
        r = pl.ds(i * chunk, chunk)
        return pltpu.make_async_copy(dy_hbm.at[r], dy_s.at[r], in_sem.at[i, 2])

    def high(i, k):
        r = pl.ds(i * chunk, chunk)
        return pltpu.make_async_copy(hi_hbm.at[k, r], far_s.at[r, pl.ds(k * half, half)], in_sem.at[i, 3 + k])

    def low(i):
        r = pl.ds(i * chunk, chunk)
        return pltpu.make_async_copy(lo_hbm.at[r], far_s.at[r], in_sem.at[i, 3])

    def fars(act):
        @pl.when(upper)
        def _():
            for k in range(2):
                act(lambda i: high(i, k))

        @pl.when(jnp.logical_not(upper))
        def _():
            act(low)

    for i in range(n):
        for copy in loads(i):
            copy.start()
        fars(lambda make: make(i).start())
    for i in range(n):
        load_dy(i).start()
    barrier = pltpu.get_barrier_semaphore()
    for peer in peers:
        pl.semaphore_signal(barrier, inc=1, device_id={"tp": peer}, device_id_type=MESH)

    def store(i):
        r = pl.ds(i * chunk, chunk)
        return pltpu.make_async_copy(dx_s.at[r], dx_hbm.at[r], out_sem.at[i])

    columns = [slice(at, at + step) for at in range(0, d, step)]

    def across_columns(v):
        return sum(v[:, at : at + 128] for at in range(0, step, 128))

    def across_rows(v):
        return sum(v[at : at + 8] for at in range(0, chunk, 8))

    scales = []
    for i in range(n):
        for copy in loads(i):
            copy.wait()
        fars(lambda make: make(i).wait())
        r = slice(i * chunk, (i + 1) * chunk)
        square = sum(across_columns(x_s[r, at].astype(F32) * x_s[r, at].astype(F32)) for at in columns)
        s = lax.rsqrt(square.sum(-1, keepdims=True) * (1 / d) + 1e-6)
        dot = jnp.zeros((chunk, 128), F32)
        for at in columns:
            xs = x_s[r, at].astype(F32) * s
            da = near_s[r, at] + far_s[r, at].astype(F32)
            prod = da * xs
            near_s[r, at] = da
            rows = across_rows(prod)
            sum_s[:, at] = rows if i == 0 else sum_s[:, at] + rows
            dot += across_columns(prod * gain_ref[:, at])
        scales.append((s, s * s * (dot.sum(-1, keepdims=True) * (1 / d))))
    part_s[...] = sum_s[...].sum(axis=0, keepdims=True)
    pl.semaphore_wait(barrier, 3)
    sends = [pltpu.make_async_remote_copy(src_ref=part_s, dst_ref=got_s.at[k], send_sem=snd.at[k], recv_sem=rcv.at[k], device_id={"tp": peer}, device_id_type=MESH) for k, peer in enumerate(peers)]
    for copy in sends:
        copy.start()
    for i, (s, m) in enumerate(scales):
        load_dy(i).wait()
        r = slice(i * chunk, (i + 1) * chunk)
        for at in columns:
            x = x_s[r, at].astype(F32)
            dx_s[r, at] = (dy_s[r, at].astype(F32) + (near_s[r, at] * gain_ref[:, at]) * s - x * m).astype(BF)
        store(i).start()
    for copy in sends:
        copy.wait()
    dgain_ref[...] = (part_s[...] + got_s[0]) + (got_s[1] + got_s[2])
    for i in range(n):
        store(i).wait()


def close(x, dy, near, hi, lo, gain, chunk=64, step=256):
    R, d = x.shape
    any_ = pl.BlockSpec(memory_space=pl.ANY)
    vmem = pl.BlockSpec(memory_space=pltpu.VMEM)
    vm = pltpu.VMEM
    return pl.pallas_call(
        functools.partial(close_kernel, chunk, step),
        in_specs=[any_] * 5 + [vmem],
        out_specs=[any_, vmem],
        out_shape=[jax.ShapeDtypeStruct((R, d), BF), jax.ShapeDtypeStruct((1, d), F32)],
        scratch_shapes=[vm((R, d), BF), vm((R, d), BF), vm((R, d), F32), vm((R, d), BF), vm((R, d), BF), vm((8, d), F32), vm((1, d), F32), vm((3, 1, d), F32),
                        pltpu.SemaphoreType.DMA((R // chunk, 5)), pltpu.SemaphoreType.DMA((R // chunk,)), pltpu.SemaphoreType.DMA((3,)), pltpu.SemaphoreType.DMA((3,))],
        compiler_params=pltpu.CompilerParams(collective_id=1, has_side_effects=True, vmem_limit_bytes=62 * 2**20),
        cost_estimate=pl.CostEstimate(flops=16 * R * d, bytes_accessed=12 * R * d, transcendentals=R),
        name="close",
    )(x, dy, near, hi, lo, gain)


def solution(mesh):
    def step(x, dy, gain, wq, wk, wv, wo):
        a, dy_all, o, dq, dkv, near, hi, lo, gain_row = main(x, dy, gain, wq, wk, wv, wo)
        got = lax.ppermute(lo, "tp", [(0, 2), (2, 0)])
        by_wq, by_wk, by_wv, by_wo = weight_gradients(a, dq, dkv, o, dy_all)
        gain_row, by_wk = lax.optimization_barrier((gain_row, by_wk))
        by_x, by_gain = close(x, dy, near, hi, got, gain_row)
        return by_x, by_gain, by_wq, by_wk, by_wv, by_wo

    tokens, columns = P(("dp", "tp"), None), P(None, "tp")
    return jax.shard_map(
        step,
        mesh=mesh,
        in_specs=(tokens, tokens, P(None), columns, columns, columns, P("tp", None)),
        out_specs=(tokens, P("dp", None), P("dp", "tp"), P("dp", "tp"), P("dp", "tp"), P(("dp", "tp"), None)),
        check_vma=False,
    )
```

```python
import functools

import jax
import jax.numpy as jnp
from jax import lax
from jax.experimental import pallas as pl
from jax.experimental.pallas import tpu as pltpu

NEG = -1e30
HIDDEN = 2 * NEG
LOG2E = 1.4426950408889634
VMEM = 56 * 2**20


def _dot(a, b, ca, cb):
    return lax.dot_general(a, b, (((ca,), (cb,)), ((), ())), preferred_element_type=jnp.float32)


from jax.sharding import PartitionSpec as P
import numpy as np

HEAD = 128
THETA = 10000
MESH = pl.DeviceIdType.MESH
F32, BF = jnp.float32, jnp.bfloat16

X0, F0, XD, YD, Y0, G0, HD, LD, ND, HI, GD = 0, 2, 4, 5, 6, 9, 12, 14, 16, 18, 20
N_REMOTE = 23
L_X, L_DY, L_G, L_COS, L_WQ, L_WK, L_WV, L_WO, L_YN, L_A0, L_Y0, L_O, L_DQ, L_DKV, L_LO, L_NEAR = 0, 1, 2, 3, 4, 5, 6, 7, 8, 9, 17, 19, 20, 21, 22, 24
N_LOCAL = 26
FINE = 32


def tables(rows):
    half = HEAD // 2
    rate = float(THETA) ** (-np.arange(half, dtype=np.float64) / half)
    place = np.concatenate([np.arange(0, rows, FINE), np.arange(FINE)]).astype(np.float64)
    angle = place[:, None] * np.concatenate([rate, rate])[None]
    return np.cos(angle).astype(np.float32), np.sin(angle).astype(np.float32)


def main_kernel(x_hbm, dy_hbm, gain_hbm, table_hbm, wq_hbm, wk_hbm, wv_hbm, wo_hbm,
                a_out, dy_out, o_out, dq_out, dkv_out, near_out, hi_out, lo_out, gain_out, scale_out, parts_out,
                a_s, dy_s, gain_1, gain_s, table_s, cos_s, sin_s, wq_s, wkv_s, wo_s, q_s, k_s, v_s, o_s, do_s, dq_s, dk32, dv32, dkv_s, lse_s, delta_s, top_s, mix_s,
                recv_s, near_recv, stage, far_x, scale_s, far_scale, sum_s, part_s, loc, snd, rcv):
    t = lax.axis_index("tp")
    chip, c = lax.div(t, 2), lax.rem(t, 2)
    partner, across = chip * 2 + 1 - c, (1 - chip) * 2 + c
    d = a_s.shape[1]
    half = d // 2
    R = x_hbm.shape[0]
    Q = R // 2
    heads = wq_hbm.shape[1] // HEAD
    cols = heads * R
    wide = 2 * R
    scale = HEAD**-0.5
    e = scale * LOG2E
    al = pl.multiple_of

    def local(src, dst, i):
        copy = pltpu.make_async_copy(src, dst, loc.at[i])
        copy.start()
        return copy

    def remote(src, dst, i, device, start=True):
        copy = pltpu.make_async_remote_copy(src_ref=src, dst_ref=dst, send_sem=snd.at[i], recv_sem=rcv.at[i], device_id={"tp": device}, device_id_type=MESH)
        if start:
            copy.start()
        return copy

    own = pl.ds(al(c * R, R), R)
    theirs = pl.ds(al((1 - c) * R, R), R)
    c_x = local(x_hbm, a_s.at[own], L_X)
    c_dy = local(dy_hbm, dy_s.at[own], L_DY)
    c_g = local(gain_hbm, gain_1, L_G)

    barrier = pltpu.get_barrier_semaphore()
    for k in range(1, 4):
        pl.semaphore_signal(barrier, inc=1, device_id={"tp": lax.rem(t + k, 4)}, device_id_type=MESH)
    pl.semaphore_wait(barrier, 3)

    def x_at(i, k):
        return pl.ds(al(2 * R + i * R + k * Q, Q), Q)

    PIECES = ((R, R), (Q, Q), (0, Q))

    def y_near(i, k):
        first, n = PIECES[i]
        return pl.ds(al(first + k * (n // 2), n // 2), n // 2)

    def y_far(i, k):
        first, n = PIECES[i]
        return pl.ds(al(2 * R + first + k * (n // 2), n // 2), n // 2)

    sends = []
    sends += [remote(x_hbm.at[pl.ds(i * Q, Q)], far_x.at[pl.ds(i * Q, Q)], X0 + i, across) for i in range(2)]
    sends += [remote(x_hbm, a_s.at[own], XD, partner), remote(dy_hbm, dy_s.at[own], YD, partner)]
    c_table = local(table_hbm, table_s, L_COS)
    c_wq = local(wq_hbm, wq_s, L_WQ)
    c_wk, c_wv = local(wk_hbm, wkv_s.at[:, pl.ds(0, HEAD)], L_WK), local(wv_hbm, wkv_s.at[:, pl.ds(HEAD, HEAD)], L_WV)
    c_wo = local(wo_hbm, wo_s, L_WO)

    def normed_rows(src, first, start, n, kept=None, place=0):
        def body(i, _):
            x = src[pl.ds(al(first + i * 16, 16), 16), :].astype(F32)
            s = lax.rsqrt(jnp.mean(x * x, -1, keepdims=True) + 1e-6)
            a_s[pl.ds(al(start + i * 16, 16), 16), :] = (x * s * gain_s[...]).astype(BF)
            if kept is not None:
                kept[pl.ds(al(place + i * 16, 16), 16), :] = jnp.broadcast_to(s, (16, HEAD))

        lax.fori_loop(0, n // 16, body, None)

    def turn(ref, n_heads, start, n):
        def body(i, _):
            r = pl.ds(al(start + i * 32, 32), 32)
            cs, sn = cos_s[r, :], sin_s[r, :]
            for h in range(n_heads):
                at = slice(h * HEAD, (h + 1) * HEAD)
                v = ref[r, at].astype(F32)
                ref[r, at] = (v * cs + pltpu.roll(v, HEAD // 2, 1) * sn).astype(BF)

        lax.fori_loop(0, n // 32, body, None)

    near0, far0 = chip * 2 * R, (1 - chip) * 2 * R

    c_dy.wait()
    remote(dy_hbm, dy_s.at[theirs], YD, partner, False).wait_recv()
    dy_ici = [remote(dy_s.at[y_near(i, c)], dy_s.at[y_far(i, c)], Y0 + i, across) for i in range(3)]
    sends += dy_ici
    c_g.wait()
    gain_s[...] = gain_1[...].astype(F32).reshape(1, d)
    c_table.wait()
    c_gain = local(gain_s, gain_out, L_COS)
    few = cos_s.shape[0] // FINE
    side = jnp.where(lax.broadcasted_iota(jnp.int32, (1, HEAD), 1) < HEAD // 2, -1.0, 1.0)

    def angles(i, _):
        r = pl.ds(al(i * FINE, FINE), FINE)
        ca, sa = table_s[0, pl.ds(i, 1), :], table_s[1, pl.ds(i, 1), :]
        cb, sb = table_s[0, few:, :], table_s[1, few:, :]
        cos_s[r, :] = ca * cb - sa * sb
        sin_s[r, :] = (sa * cb + ca * sb) * side

    lax.fori_loop(0, few, angles, None)
    c_x.wait()
    remote(x_hbm, a_s.at[theirs], XD, partner, False).wait_recv()

    def a_copy(i, k):
        token = jnp.where(i < 2, near0 + i * R + k * Q, far0 + (i - 2) * Q + k * R)
        return pltpu.make_async_copy(a_s.at[pl.ds(al(i * R + k * Q, Q), Q)], a_out.at[pl.ds(al(token, Q), Q)], loc.at[L_A0 + 2 * i + k])

    def project_block(i, _):
        @pl.when(i >= 2)
        def _():
            j = i - 2
            landed = far_x.at[pl.ds(al(j * Q, Q), Q)]
            remote(x_hbm.at[pl.ds(0, Q)], landed, X0 + j, across, False).wait_recv()
            give = remote(landed, a_s.at[x_at(j, c)], F0 + j, partner)
            normed_rows(far_x, j * Q, 2 * R + j * R + c * Q, Q, far_scale, j * Q)
            remote(landed, a_s.at[x_at(j, 1 - c)], F0 + j, partner, False).wait_recv()
            normed_rows(a_s, 2 * R + j * R + (1 - c) * Q, 2 * R + j * R + (1 - c) * Q, Q)
            give.wait_send()

        @pl.when(i < 2)
        def _():
            normed_rows(a_s, i * R, i * R, R, scale_s, i * R)

        for k in range(2):
            a_copy(i, k).start()

        @pl.when(i == 0)
        def _():
            for w in (c_wq, c_wk, c_wv):
                w.wait()

        block = pl.ds(al(i * R, R), R)
        r = _dot(a_s[block, :], wq_s[...], 1, 0).astype(BF)
        kv = _dot(a_s[block, :], wkv_s[...], 1, 0).astype(BF)
        for k in range(2):
            token = jnp.where(i < 2, near0 + i * R + k * Q, far0 + (i - 2) * Q + k * R)
            p = pl.ds(al(token, Q), Q)
            q_s[p, :] = r[k * Q : (k + 1) * Q]
            k_s[p, :] = kv[k * Q : (k + 1) * Q, :HEAD]
            v_s[p, :] = kv[k * Q : (k + 1) * Q, HEAD:]
            turn(q_s, heads, token, Q)
            turn(k_s, 1, token, Q)

        @pl.when(i < 2)
        def _():
            @pl.when(i == 0)
            def _():
                c_wo.wait()

            do_s[pl.ds(al(near0 + i * R, R), R), :] = _dot(dy_s[block, :], wo_s[...], 1, 1).astype(BF)

    sum_s[...] = jnp.zeros_like(sum_s)
    dk32[...] = jnp.zeros_like(dk32)
    dv32[...] = jnp.zeros_like(dv32)
    lax.fori_loop(0, 4, project_block, None)
    c_yn = local(dy_s.at[pl.ds(0, 2 * R)], dy_out.at[pl.ds(al(near0, 2 * R), 2 * R)], L_YN)

    def seen_mask():
        return lax.rem(lax.broadcasted_iota(jnp.int32, (R, wide), 1), R) >= lax.broadcasted_iota(jnp.int32, (R, wide), 0)

    strips = range(0, cols, wide)

    def strip(ref, rows, at):
        h = at // R
        return jnp.concatenate([ref[rows, (h + n) * HEAD : (h + n + 1) * HEAD] for n in range(wide // R)], axis=0)

    def attend_block(b, _):
        rows = pl.ds(al(b * R, R), R)
        top_s[...] = jnp.full(top_s.shape, NEG, F32)
        mix_s[...] = jnp.zeros_like(mix_s)

        def pair(j, masked):
            here = pl.ds(al(j * R, R), R)
            keys = k_s[here, :]
            values = jnp.concatenate([v_s[here, :].T, jnp.ones((8, R), BF)], axis=0)
            scores = [_dot(keys, strip(q_s, rows, at), 1, 1) for at in strips]
            weights, keeps = [], []
            for at, s in zip(strips, scores):
                if masked:
                    s = jnp.where(seen_mask(), s, HIDDEN)
                old = top_s[:, at : at + wide]
                top = jnp.maximum(old, s.max(axis=0, keepdims=True))
                top_s[:, at : at + wide] = top
                weights.append(jnp.exp2((s - top) * e).astype(BF))
                keeps.append(jnp.exp2((old - top) * e))
            for at, p, keep in zip(strips, weights, keeps):
                mix_s[:, at : at + wide] = mix_s[:, at : at + wide] * keep + _dot(values, p, 1, 0)

        lax.fori_loop(0, b, lambda j, _: pair(j, False), None)
        pair(b, True)
        total = mix_s[HEAD : HEAD + 1, :]
        out = (mix_s[:HEAD, :] * (1 / total)).T.astype(BF)
        for h in range(heads):
            o_s[rows, h * HEAD : (h + 1) * HEAD] = out[h * R : (h + 1) * R]
        lse_s[b] = top_s[...] * scale + jnp.log(total)

    lax.fori_loop(0, 4, attend_block, None)
    c_o = local(o_s, o_out, L_O)

    def backward_block(b, first=None):
        n, first = (R, 0) if first is None else (Q, first)
        rows = pl.ds(al(b * R + first, n), n)
        per = wide // n
        parts = [(h, slice(h * n, h * n + wide)) for h in range(0, heads, per)]

        def of(ref, h):
            return jnp.concatenate([ref[rows, (h + m) * HEAD : (h + m + 1) * HEAD] for m in range(per)], axis=0)

        for h, at in parts:
            both = of(do_s, h).astype(F32) * of(o_s, h).astype(F32)
            delta_s[:, at] = both.T.sum(axis=0, keepdims=True)
            top_s[:, at] = jnp.concatenate([lse_s[b, :, (h + m) * R + first : (h + m) * R + first + n] for m in range(per)], axis=1) * LOG2E
        mix_s[...] = jnp.zeros_like(mix_s)

        def pair(j, masked):
            here = pl.ds(al(j * R, R), R)
            keys, values = k_s[here, :], v_s[here, :]
            keys_t = keys.T
            dv = dk = None
            for h, at in parts:
                q, do = of(q_s, h), of(do_s, h)
                p = jnp.exp2(_dot(keys, q, 1, 1) * e - top_s[:, at])
                if masked:
                    seen = lax.rem(lax.broadcasted_iota(jnp.int32, (R, wide), 1), n) + first >= lax.broadcasted_iota(jnp.int32, (R, wide), 0)
                    p = jnp.where(seen, p, 0.0)
                ds = (p * (_dot(values, do, 1, 1) - delta_s[:, at])).astype(BF)
                a, g = _dot(p.astype(BF), do, 1, 0), _dot(ds, q, 1, 0)
                dv, dk = (a, g) if dv is None else (dv + a, dk + g)
                mix_s[:HEAD, at] += _dot(keys_t, ds, 1, 0)
            dv32[here, :] += dv
            dk32[here, :] += dk

        lax.fori_loop(0, b, lambda j, _: pair(j, False), None)
        pair(b, True)
        out = (mix_s[:HEAD, : heads * n] * scale).T
        cs, sn = cos_s[rows, :], sin_s[rows, :]
        for h in range(heads):
            g = out[h * n : (h + 1) * n]
            dq_s[rows, h * HEAD : (h + 1) * HEAD] = (g * cs - pltpu.roll(g, HEAD // 2, 1) * sn).astype(BF)

    def keys_done(b):
        rows = pl.ds(al(b * R, R), R)
        g = dk32[rows, :] * scale
        dkv_s[rows, :HEAD] = (g * cos_s[rows, :] - pltpu.roll(g, HEAD // 2, 1) * sin_s[rows, :]).astype(BF)
        dkv_s[rows, HEAD:] = dv32[rows, :].astype(BF)

    def term(b, k):
        rows, at = pl.ds(al(b * R, R), R), pl.ds(al(k * half, half), half)
        return _dot(dq_s[rows, :], wq_s[at, :], 1, 1) + _dot(dkv_s[rows, :], wkv_s[at, :], 1, 1)

    def dy_copy(i, b):
        return pltpu.make_async_copy(dy_s.at[pl.ds(al(2 * R + (1 - i) * R, R), R)], dy_out.at[pl.ds(al(b * R, R), R)], loc.at[L_Y0 + i])

    def give_hi(k):
        return remote(a_s.at[pl.ds(0, R), pl.ds(al(k * half, half), half)], recv_s.at[k], HD + k, partner, False)

    def hi_copy(k):
        return remote(a_s.at[pl.ds(0, R), pl.ds(al(k * half, half), half)], hi_out.at[k], HI + k, across, False)

    def add_up(k, got, x, scales, first, give=None):
        s = scales[pl.ds(al(first, R), R), :]
        for at in range(0, half, HEAD):
            col = pl.ds(al(k * half + at, HEAD), HEAD)
            v = stage[k, :, at : at + HEAD] + got(at, col).astype(F32)
            if give is None:
                stage[k, :, at : at + HEAD] = v
            else:
                a_s[give, col] = v.astype(BF)
            v = v * (x[:, col].astype(F32) * s)
            sum_s[:, col] += sum(v[r : r + 8] for r in range(0, R, 8))

    far_hi, far_lo = (1 - chip) * 2 + 1, (1 - chip) * 2

    def pass_on(i):
        dy_ici[i].wait_recv()
        remote(dy_s.at[y_far(i, c)], dy_s.at[y_far(i, c)], G0 + i, partner)

    def piece(i, b):
        first, n = PIECES[i]
        remote(dy_s.at[y_far(i, 1 - c)], dy_s.at[y_far(i, 1 - c)], G0 + i, partner, False).wait_recv()
        do_s[pl.ds(al(b * R + first % R, n), n), :] = _dot(dy_s[pl.ds(2 * R + first, n), :], wo_s[...], 1, 1).astype(BF)

    own_x = pltpu.make_async_copy(x_hbm, a_s.at[pl.ds(3 * R, R)], loc.at[L_X])

    def backward_step(s, _):
        @pl.when(s == 1)
        def _():
            pass_on(0)

        @pl.when(s == 2)
        def _():
            for k in range(4):
                for n in range(2):
                    a_copy(k, n).wait()
            c_gain.wait()
            own_x.start()
            piece(0, far_hi)
            dy_copy(0, far_hi).start()

        backward_block(jnp.where(s < 2, chip * 2 + 1 - s, far_hi))

        @pl.when(s == 2)
        def _():
            pass_on(1)
            keys_done(far_hi)

            def hi_part(k, _):
                @pl.when(c == 0)
                def _():
                    a_s[pl.ds(0, R), pl.ds(al(k * half, half), half)] = term(far_hi, k).astype(BF)
                    give_hi(k).start()

                @pl.when(c == 1)
                def _():
                    stage[k] = term(far_hi, k)

            lax.fori_loop(0, 2, hi_part, None)

            def hi_sum(k, _):
                give_hi(k).wait_recv()
                add_up(k, lambda at, col: recv_s[k, :, at : at + HEAD], far_x, far_scale, 0, pl.ds(0, R))
                hi_copy(k).start()

            @pl.when(c == 1)
            def _():
                lax.fori_loop(0, 2, hi_sum, None)

    lax.fori_loop(0, 3, backward_step, None)
    piece(1, far_lo)

    @pl.when(c == 1)
    def _():
        pass_on(2)

    backward_block(far_lo, Q)

    @pl.when(c == 0)
    def _():
        pass_on(2)

    piece(2, far_lo)
    dy_copy(1, far_lo).start()
    backward_block(far_lo, 0)
    keys_done(far_lo)
    c_dq = local(dq_s, dq_out, L_DQ)
    keys_done(chip * 2)
    keys_done(chip * 2 + 1)
    c_dkv = local(dkv_s, dkv_out, L_DKV)

    def place(i, k):
        return pl.ds(al(R + i * R, R), R), pl.ds(al(k * half, half), half)

    def give_half(i, k):
        rows, at = place(i, k)
        return remote(a_s.at[rows, at], near_recv.at[:, at] if i == 0 else recv_s.at[k], (ND if i == 0 else LD) + k, partner, False)

    def lo_copy(k):
        rows, at = place(1, k)
        return pltpu.make_async_copy(a_s.at[rows, at], lo_out.at[:, at], loc.at[L_LO + k])

    def near_copy(k):
        return pltpu.make_async_copy(stage.at[k], near_out.at[:, pl.ds(al(k * half, half), half)], loc.at[L_NEAR + k])

    def give_part(n, _):
        k, low = lax.rem(n, 2), lax.div(n, 2) != c
        b = jnp.where(low, (1 - chip) * 2, chip * 2 + 1 - c)

        @pl.when(low & (c == 0))
        def _():
            rows, at = place(1, k)
            stage[k] = term(b, k)
            give_half(1, k).wait_recv()
            add_up(k, lambda at, col: recv_s[k, :, at : at + HEAD], far_x, far_scale, 0, rows)
            lo_copy(k).start()

        @pl.when(jnp.logical_not(low & (c == 0)))
        def _():
            rows, at = place(jnp.where(low, 1, 0), k)
            a_s[rows, at] = term(b, k).astype(BF)

            @pl.when(low)
            def _():
                give_half(1, k).start()

            @pl.when(jnp.logical_not(low))
            def _():
                give_half(0, k).start()

    lax.fori_loop(0, 4, give_part, None)

    own_x.wait()

    def own_part(k, _):
        stage[k] = term(chip * 2 + c, k)
        give_half(0, k).wait_recv()
        add_up(k, lambda at, col: near_recv[:, col], a_s.at[pl.ds(3 * R, R)], scale_s, c * R)
        near_copy(k).start()

    lax.fori_loop(0, 2, own_part, None)
    part_s[...] = sum_s[...].sum(axis=0, keepdims=True)
    gives = [remote(part_s, parts_out.at[k], GD + k, peer) for k, peer in enumerate((partner, across, (1 - chip) * 2 + 1 - c))]
    c_part = local(part_s, parts_out.at[3], L_X)
    c_scale = local(scale_s.at[pl.ds(al(c * R, R), R)], scale_out, L_G)

    @pl.when(c == 1)
    def _():
        for k in range(2):
            hi_copy(k).wait()
            give_half(1, k).wait_send()

    @pl.when(c == 0)
    def _():
        for k in range(2):
            lo_copy(k).wait()
            give_hi(k).wait_send()

    for i in range(3):
        remote(dy_s.at[y_far(i, c)], dy_s.at[y_far(i, c)], G0 + i, partner, False).wait_send()
    for i in range(2):
        dy_copy(i, far_hi if i == 0 else far_lo).wait()
        give_half(0, i).wait_send()
        near_copy(i).wait()
    for copy in gives:
        copy.wait()
    for copy in sends:
        copy.wait_send()
    for copy in (c_o, c_yn, c_dq, c_dkv, c_scale, c_part):
        copy.wait()


def main(x, dy, gain, wq, wk, wv, wo):
    R, d = x.shape
    n, width = 4 * R, wq.shape[1]
    heads = width // HEAD
    table = jnp.asarray(np.stack(tables(n)))
    any_ = pl.BlockSpec(memory_space=pl.ANY)
    vm = pltpu.VMEM
    flops = 2 * n * d * (3 * width + 4 * HEAD) + 7 * n * n * width
    return pl.pallas_call(
        main_kernel,
        in_specs=[any_] * 8,
        out_specs=[any_] * 11,
        out_shape=[jax.ShapeDtypeStruct((n, d), BF), jax.ShapeDtypeStruct((n, d), BF), jax.ShapeDtypeStruct((n, width), BF), jax.ShapeDtypeStruct((n, width), BF),
                   jax.ShapeDtypeStruct((n, 2 * HEAD), BF), jax.ShapeDtypeStruct((R, d), F32), jax.ShapeDtypeStruct((2, R, d // 2), BF), jax.ShapeDtypeStruct((R, d), BF), jax.ShapeDtypeStruct((1, d), F32), jax.ShapeDtypeStruct((R, HEAD), F32), jax.ShapeDtypeStruct((4, 1, d), F32)],
        scratch_shapes=[vm((n, d), BF), vm((n, d), BF), vm((d,), BF), vm((1, d), F32), vm(table.shape, F32), vm((n, HEAD), F32), vm((n, HEAD), F32), vm((d, width), BF), vm((d, 2 * HEAD), BF), vm((width, d), BF),
                        vm((n, width), BF), vm((n, HEAD), BF), vm((n, HEAD), BF), vm((n, width), BF), vm((n, width), BF), vm((n, width), BF),
                        vm((n, HEAD), F32), vm((n, HEAD), F32), vm((n, 2 * HEAD), BF), vm((4, 1, heads * R), F32), vm((1, heads * R), F32), vm((1, heads * R), F32), vm((HEAD + 8, heads * R), F32),
                        vm((2, R, d // 2), BF), vm((R, d), BF), vm((2, R, d // 2), F32),
                        vm((R, d), BF), vm((2 * R, HEAD), F32), vm((R, HEAD), F32), vm((8, d), F32), vm((1, d), F32),
                        pltpu.SemaphoreType.DMA((N_LOCAL,)), pltpu.SemaphoreType.DMA((N_REMOTE,)), pltpu.SemaphoreType.DMA((N_REMOTE,))],
        compiler_params=pltpu.CompilerParams(collective_id=0, has_side_effects=True, vmem_limit_bytes=67043328),
        cost_estimate=pl.CostEstimate(flops=flops, bytes_accessed=60 * 2**20, transcendentals=n * n * heads),
        name="main",
    )(x, dy, gain, table, wq, wk, wv, wo)


def row_scale(x):
    return lax.rsqrt(jnp.mean(x * x, -1, keepdims=True) + 1e-6)


def weights_kernel(a_ref, dq_ref, dkv_ref, o_ref, dy_ref, wq_ref, wk_ref, wv_ref, wo_ref):
    a = a_ref[...]
    wq_ref[...] = _dot(a, dq_ref[...], 0, 0).astype(BF)
    kv = _dot(a, dkv_ref[...], 0, 0).astype(BF)
    wk_ref[...] = kv[:, :HEAD]
    wv_ref[...] = kv[:, HEAD:]
    wo_ref[...] = _dot(o_ref[...], dy_ref[...], 0, 0).astype(BF)


def weight_gradients(a, dq, dkv, o, dy, tile=512):
    n, d = a.shape
    width = dq.shape[1]
    tall = pl.BlockSpec((n, tile), lambda i: (0, i))
    whole = lambda w: pl.BlockSpec((n, w), lambda i: (0, 0))
    rows = lambda w: pl.BlockSpec((tile, w), lambda i: (i, 0))
    return pl.pallas_call(
        weights_kernel,
        grid=(d // tile,),
        in_specs=[tall, whole(width), whole(2 * HEAD), whole(width), tall],
        out_specs=[rows(width), rows(HEAD), rows(HEAD), pl.BlockSpec((width, tile), lambda i: (0, i))],
        out_shape=[jax.ShapeDtypeStruct((d, width), BF), jax.ShapeDtypeStruct((d, HEAD), BF), jax.ShapeDtypeStruct((d, HEAD), BF), jax.ShapeDtypeStruct((width, d), BF)],
        compiler_params=pltpu.CompilerParams(dimension_semantics=("arbitrary",), vmem_limit_bytes=62 * 2**20),
        cost_estimate=pl.CostEstimate(flops=2 * n * d * (2 * width + 2 * HEAD), bytes_accessed=2 * (2 * n * d + 2 * n * width + 2 * d * width), transcendentals=0),
        name="weights",
    )(a, dq, dkv, o, dy)


def close_kernel(chunk, x_hbm, dy_hbm, near_hbm, hi_hbm, lo_hbm, gain_hbm, scale_hbm, parts_hbm, dx_hbm, dgain_hbm, x_s, dy_s, near_s, far_s, dx_s, gain_s, scale_s, parts_s, dgain_s, in_sem, out_sem):
    R, d = x_s.shape
    half = d // 2
    upper = lax.rem(lax.axis_index("tp"), 2) == 1
    n = R // chunk

    def loads(i):
        r = pl.ds(i * chunk, chunk)
        return [pltpu.make_async_copy(src.at[r], dst.at[r], in_sem.at[i, k]) for k, (src, dst) in enumerate(((x_hbm, x_s), (near_hbm, near_s), (dy_hbm, dy_s)))]

    def high(i, k):
        r = pl.ds(i * chunk, chunk)
        return pltpu.make_async_copy(hi_hbm.at[k, r], far_s.at[r, pl.ds(k * half, half)], in_sem.at[i, 3 + k])

    def low(i):
        r = pl.ds(i * chunk, chunk)
        return pltpu.make_async_copy(lo_hbm.at[r], far_s.at[r], in_sem.at[i, 3])

    def fars(act):
        @pl.when(upper)
        def _():
            for k in range(2):
                act(lambda i: high(i, k))

        @pl.when(jnp.logical_not(upper))
        def _():
            act(low)

    small = [pltpu.make_async_copy(src, dst, out_sem.at[n + k]) for k, (src, dst) in enumerate(((gain_hbm, gain_s), (scale_hbm, scale_s), (parts_hbm, parts_s)))]
    for copy in small:
        copy.start()
    for i in range(n):
        for copy in loads(i):
            copy.start()
        fars(lambda make: make(i).start())

    def store(i):
        r = pl.ds(i * chunk, chunk)
        return pltpu.make_async_copy(dx_s.at[r], dx_hbm.at[r], out_sem.at[i])

    columns = [slice(at, at + HEAD) for at in range(0, d, HEAD)]
    for copy in small:
        copy.wait()
    dgain_s[...] = (parts_s[3] + parts_s[0]) + (parts_s[1] + parts_s[2])
    give_gain = pltpu.make_async_copy(dgain_s, dgain_hbm, out_sem.at[n])
    give_gain.start()
    for i in range(n):
        for copy in loads(i):
            copy.wait()
        fars(lambda make: make(i).wait())
        r = slice(i * chunk, (i + 1) * chunk)
        s = scale_s[r, :]
        dot = jnp.zeros((chunk, HEAD), F32)
        for at in columns:
            g = (near_s[r, at] + far_s[r, at].astype(F32)) * gain_s[:, at]
            near_s[r, at] = g
            dot += g * x_s[r, at].astype(F32)
        m = s * s * s * (dot.sum(-1, keepdims=True) * (1 / d))
        for at in columns:
            dx_s[r, at] = (dy_s[r, at].astype(F32) + near_s[r, at] * s - x_s[r, at].astype(F32) * m).astype(BF)
        store(i).start()
    give_gain.wait()
    for i in range(n):
        store(i).wait()


def close(x, dy, near, hi, lo, gain, scale, parts, chunk=64):
    R, d = x.shape
    hbm = pl.BlockSpec(memory_space=pltpu.HBM)
    vm = pltpu.VMEM
    return pl.pallas_call(
        functools.partial(close_kernel, chunk),
        in_specs=[hbm] * 8,
        out_specs=[hbm] * 2,
        out_shape=[jax.ShapeDtypeStruct((R, d), BF), jax.ShapeDtypeStruct((1, d), F32)],
        scratch_shapes=[vm((R, d), BF), vm((R, d), BF), vm((R, d), F32), vm((R, d), BF), vm((R, d), BF), vm((1, d), F32), vm((R, HEAD), F32), vm((4, 1, d), F32), vm((1, d), F32),
                        pltpu.SemaphoreType.DMA((R // chunk, 5)), pltpu.SemaphoreType.DMA((R // chunk + 3,))],
        compiler_params=pltpu.CompilerParams(vmem_limit_bytes=62 * 2**20),
        cost_estimate=pl.CostEstimate(flops=16 * R * d, bytes_accessed=12 * R * d, transcendentals=R),
        name="close",
    )(x, dy, near, hi, lo, gain, scale, parts)


def solution(mesh):
    def step(x, dy, gain, wq, wk, wv, wo):
        a, dy_all, o, dq, dkv, near, hi, lo, gain_row, scale, parts = main(x, dy, gain, wq, wk, wv, wo)
        got = lax.ppermute(lo, "tp", [(0, 2), (2, 0)])
        by_wq, by_wk, by_wv, by_wo = weight_gradients(a, dq, dkv, o, dy_all)
        gain_row, by_wk = lax.optimization_barrier((gain_row, by_wk))
        by_x, by_gain = close(x, dy, near, hi, got, gain_row, scale, parts)
        return by_x, by_gain, by_wq, by_wk, by_wv, by_wo

    tokens, columns = P(("dp", "tp"), None), P(None, "tp")
    return jax.shard_map(
        step,
        mesh=mesh,
        in_specs=(tokens, tokens, P(None), columns, columns, columns, P("tp", None)),
        out_specs=(tokens, P("dp", None), P("dp", "tp"), P("dp", "tp"), P("dp", "tp"), P(("dp", "tp"), None)),
        check_vma=False,
    )
```

```python
import functools

import jax
import jax.numpy as jnp
from jax import lax
from jax.experimental import pallas as pl
from jax.experimental.pallas import tpu as pltpu

NEG = -1e30
HIDDEN = 2 * NEG
LOG2E = 1.4426950408889634
VMEM = 56 * 2**20


def _dot(a, b, ca, cb):
    return lax.dot_general(a, b, (((ca,), (cb,)), ((), ())), preferred_element_type=jnp.float32)


from jax.sharding import PartitionSpec as P
import numpy as np

HEAD = 128
THETA = 10000
MESH = pl.DeviceIdType.MESH
F32, BF = jnp.float32, jnp.bfloat16

X0, F0, XD, YD, Y0, G0, HD, LD, ND, HI, GD = 0, 2, 4, 5, 6, 9, 12, 14, 16, 18, 20
N_REMOTE = 23
L_X, L_DY, L_G, L_COS, L_WQ, L_WK, L_WV, L_WO, L_YN, L_A0, L_Y0, L_O, L_DQ, L_DKV, L_LO, L_NEAR = 0, 1, 2, 3, 4, 5, 6, 7, 8, 9, 17, 19, 20, 21, 22, 24
N_LOCAL = 26
FINE = 32


def tables(rows):
    half = HEAD // 2
    rate = float(THETA) ** (-np.arange(half, dtype=np.float64) / half)
    place = np.concatenate([np.arange(0, rows, FINE), np.arange(FINE)]).astype(np.float64)
    angle = place[:, None] * np.concatenate([rate, rate])[None]
    return np.cos(angle).astype(np.float32), np.sin(angle).astype(np.float32)


def main_kernel(x_hbm, dy_hbm, gain_hbm, table_hbm, wq_hbm, wk_hbm, wv_hbm, wo_hbm,
                a_out, dy_out, o_out, dq_out, dkv_out, near_out, hi_out, lo_out, gain_out, scale_out, parts_out,
                a_s, dy_s, gain_1, gain_s, table_s, cos_s, sin_s, wq_s, wkv_s, wo_s, q_s, k_s, v_s, o_s, do_s, dq_s, dk32, dv32, dkv_s, lse_s, delta_s, top_s, mix_s,
                recv_s, near_recv, stage, far_x, scale_s, far_scale, sum_s, part_s, loc, snd, rcv):
    t = lax.axis_index("tp")
    chip, c = lax.div(t, 2), lax.rem(t, 2)
    partner, across = chip * 2 + 1 - c, (1 - chip) * 2 + c
    d = a_s.shape[1]
    half = d // 2
    R = x_hbm.shape[0]
    Q = R // 2
    heads = wq_hbm.shape[1] // HEAD
    cols = heads * R
    wide = 2 * R
    scale = HEAD**-0.5
    e = scale * LOG2E
    al = pl.multiple_of

    def local(src, dst, i):
        copy = pltpu.make_async_copy(src, dst, loc.at[i])
        copy.start()
        return copy

    def remote(src, dst, i, device, start=True):
        copy = pltpu.make_async_remote_copy(src_ref=src, dst_ref=dst, send_sem=snd.at[i], recv_sem=rcv.at[i], device_id={"tp": device}, device_id_type=MESH)
        if start:
            copy.start()
        return copy

    own = pl.ds(al(c * R, R), R)
    theirs = pl.ds(al((1 - c) * R, R), R)
    c_x = local(x_hbm, a_s.at[own], L_X)
    c_dy = local(dy_hbm, dy_s.at[own], L_DY)
    c_g = local(gain_hbm, gain_1, L_G)

    barrier = pltpu.get_barrier_semaphore()
    for k in range(1, 4):
        pl.semaphore_signal(barrier, inc=1, device_id={"tp": lax.rem(t + k, 4)}, device_id_type=MESH)
    pl.semaphore_wait(barrier, 3)

    def x_at(i, k):
        return pl.ds(al(2 * R + i * R + k * Q, Q), Q)

    PIECES = ((R, R), (Q, Q), (0, Q))

    def y_near(i, k):
        first, n = PIECES[i]
        return pl.ds(al(first + k * (n // 2), n // 2), n // 2)

    def y_far(i, k):
        first, n = PIECES[i]
        return pl.ds(al(2 * R + first + k * (n // 2), n // 2), n // 2)

    sends = []
    sends += [remote(x_hbm.at[pl.ds(i * Q, Q)], far_x.at[pl.ds(i * Q, Q)], X0 + i, across) for i in range(2)]
    sends += [remote(x_hbm, a_s.at[own], XD, partner), remote(dy_hbm, dy_s.at[own], YD, partner)]
    c_table = local(table_hbm, table_s, L_COS)
    c_wq = local(wq_hbm, wq_s, L_WQ)
    c_wk, c_wv = local(wk_hbm, wkv_s.at[:, pl.ds(0, HEAD)], L_WK), local(wv_hbm, wkv_s.at[:, pl.ds(HEAD, HEAD)], L_WV)
    c_wo = local(wo_hbm, wo_s, L_WO)

    def normed_rows(src, first, start, n, kept=None, place=0):
        def body(i, _):
            x = src[pl.ds(al(first + i * 16, 16), 16), :].astype(F32)
            s = lax.rsqrt(jnp.mean(x * x, -1, keepdims=True) + 1e-6)
            a_s[pl.ds(al(start + i * 16, 16), 16), :] = (x * s * gain_s[...]).astype(BF)
            if kept is not None:
                kept[pl.ds(al(place + i * 16, 16), 16), :] = jnp.broadcast_to(s, (16, HEAD))

        lax.fori_loop(0, n // 16, body, None)

    def turn(ref, n_heads, start, n):
        def body(i, _):
            r = pl.ds(al(start + i * 32, 32), 32)
            cs, sn = cos_s[r, :], sin_s[r, :]
            for h in range(n_heads):
                at = slice(h * HEAD, (h + 1) * HEAD)
                v = ref[r, at].astype(F32)
                ref[r, at] = (v * cs + pltpu.roll(v, HEAD // 2, 1) * sn).astype(BF)

        lax.fori_loop(0, n // 32, body, None)

    near0, far0 = chip * 2 * R, (1 - chip) * 2 * R

    c_dy.wait()
    remote(dy_hbm, dy_s.at[theirs], YD, partner, False).wait_recv()
    dy_ici = [remote(dy_s.at[y_near(i, c)], dy_s.at[y_far(i, c)], Y0 + i, across) for i in range(3)]
    sends += dy_ici
    c_g.wait()
    gain_s[...] = gain_1[...].astype(F32).reshape(1, d)
    c_table.wait()
    c_gain = local(gain_s, gain_out, L_COS)
    few = cos_s.shape[0] // FINE
    side = jnp.where(lax.broadcasted_iota(jnp.int32, (1, HEAD), 1) < HEAD // 2, -1.0, 1.0)

    def angles(i, _):
        r = pl.ds(al(i * FINE, FINE), FINE)
        ca, sa = table_s[0, pl.ds(i, 1), :], table_s[1, pl.ds(i, 1), :]
        cb, sb = table_s[0, few:, :], table_s[1, few:, :]
        cos_s[r, :] = ca * cb - sa * sb
        sin_s[r, :] = (sa * cb + ca * sb) * side

    lax.fori_loop(0, few, angles, None)
    c_x.wait()
    remote(x_hbm, a_s.at[theirs], XD, partner, False).wait_recv()

    def a_copy(i, k):
        token = jnp.where(i < 2, near0 + i * R + k * Q, far0 + (i - 2) * Q + k * R)
        return pltpu.make_async_copy(a_s.at[pl.ds(al(i * R + k * Q, Q), Q)], a_out.at[pl.ds(al(token, Q), Q)], loc.at[L_A0 + 2 * i + k])

    def project_block(i, _):
        @pl.when(i >= 2)
        def _():
            j = i - 2
            landed = far_x.at[pl.ds(al(j * Q, Q), Q)]
            remote(x_hbm.at[pl.ds(0, Q)], landed, X0 + j, across, False).wait_recv()
            give = remote(landed, a_s.at[x_at(j, c)], F0 + j, partner)
            normed_rows(far_x, j * Q, 2 * R + j * R + c * Q, Q, far_scale, j * Q)
            remote(landed, a_s.at[x_at(j, 1 - c)], F0 + j, partner, False).wait_recv()
            normed_rows(a_s, 2 * R + j * R + (1 - c) * Q, 2 * R + j * R + (1 - c) * Q, Q)
            give.wait_send()

        @pl.when(i < 2)
        def _():
            normed_rows(a_s, i * R, i * R, R, scale_s, i * R)

        for k in range(2):
            a_copy(i, k).start()

        @pl.when(i == 0)
        def _():
            for w in (c_wq, c_wk, c_wv):
                w.wait()

        block = pl.ds(al(i * R, R), R)
        r = _dot(a_s[block, :], wq_s[...], 1, 0).astype(BF)
        kv = _dot(a_s[block, :], wkv_s[...], 1, 0).astype(BF)
        for k in range(2):
            token = jnp.where(i < 2, near0 + i * R + k * Q, far0 + (i - 2) * Q + k * R)
            p = pl.ds(al(token, Q), Q)
            q_s[p, :] = r[k * Q : (k + 1) * Q]
            k_s[p, :] = kv[k * Q : (k + 1) * Q, :HEAD]
            v_s[p, :] = kv[k * Q : (k + 1) * Q, HEAD:]
            turn(q_s, heads, token, Q)
            turn(k_s, 1, token, Q)

        @pl.when(i < 2)
        def _():
            @pl.when(i == 0)
            def _():
                c_wo.wait()

            do_s[pl.ds(al(near0 + i * R, R), R), :] = _dot(dy_s[block, :], wo_s[...], 1, 1).astype(BF)

    sum_s[...] = jnp.zeros_like(sum_s)
    dk32[...] = jnp.zeros_like(dk32)
    dv32[...] = jnp.zeros_like(dv32)
    lax.fori_loop(0, 4, project_block, None)
    c_yn = local(dy_s.at[pl.ds(0, 2 * R)], dy_out.at[pl.ds(al(near0, 2 * R), 2 * R)], L_YN)

    def seen_mask():
        return lax.rem(lax.broadcasted_iota(jnp.int32, (R, wide), 1), R) >= lax.broadcasted_iota(jnp.int32, (R, wide), 0)

    strips = range(0, cols, wide)

    def strip(ref, rows, at):
        h = at // R
        return jnp.concatenate([ref[rows, (h + n) * HEAD : (h + n + 1) * HEAD] for n in range(wide // R)], axis=0)

    def attend_block(b, _):
        rows = pl.ds(al(b * R, R), R)
        top_s[...] = jnp.full(top_s.shape, NEG, F32)
        mix_s[...] = jnp.zeros_like(mix_s)

        def pair(j, masked):
            here = pl.ds(al(j * R, R), R)
            keys = k_s[here, :]
            values = jnp.concatenate([v_s[here, :].T, jnp.ones((8, R), BF)], axis=0)
            scores = [_dot(keys, strip(q_s, rows, at), 1, 1) for at in strips]
            weights, keeps = [], []
            for at, s in zip(strips, scores):
                if masked:
                    s = jnp.where(seen_mask(), s, HIDDEN)
                old = top_s[:, at : at + wide]
                top = jnp.maximum(old, s.max(axis=0, keepdims=True))
                top_s[:, at : at + wide] = top
                weights.append(jnp.exp2((s - top) * e).astype(BF))
                keeps.append(jnp.exp2((old - top) * e))
            for at, p, keep in zip(strips, weights, keeps):
                mix_s[:, at : at + wide] = mix_s[:, at : at + wide] * keep + _dot(values, p, 1, 0)

        lax.fori_loop(0, b, lambda j, _: pair(j, False), None)
        pair(b, True)
        total = mix_s[HEAD : HEAD + 1, :]
        out = (mix_s[:HEAD, :] * (1 / total)).T.astype(BF)
        for h in range(heads):
            o_s[rows, h * HEAD : (h + 1) * HEAD] = out[h * R : (h + 1) * R]
        lse_s[b] = top_s[...] * scale + jnp.log(total)

    lax.fori_loop(0, 4, attend_block, None)
    c_o = local(o_s, o_out, L_O)

    def backward_block(b, first=None):
        n, first = (R, 0) if first is None else (Q, first)
        rows = pl.ds(al(b * R + first, n), n)
        per = wide // n
        parts = [(h, slice(h * n, h * n + wide)) for h in range(0, heads, per)]

        def of(ref, h):
            return jnp.concatenate([ref[rows, (h + m) * HEAD : (h + m + 1) * HEAD] for m in range(per)], axis=0)

        for h, at in parts:
            both = of(do_s, h).astype(F32) * of(o_s, h).astype(F32)
            delta_s[:, at] = both.T.sum(axis=0, keepdims=True)
            top_s[:, at] = jnp.concatenate([lse_s[b, :, (h + m) * R + first : (h + m) * R + first + n] for m in range(per)], axis=1) * LOG2E
        mix_s[...] = jnp.zeros_like(mix_s)

        def pair(j, masked):
            here = pl.ds(al(j * R, R), R)
            keys, values = k_s[here, :], v_s[here, :]
            keys_t = keys.T
            dv = dk = None
            for h, at in parts:
                q, do = of(q_s, h), of(do_s, h)
                p = jnp.exp2(_dot(keys, q, 1, 1) * e - top_s[:, at])
                if masked:
                    seen = lax.rem(lax.broadcasted_iota(jnp.int32, (R, wide), 1), n) + first >= lax.broadcasted_iota(jnp.int32, (R, wide), 0)
                    p = jnp.where(seen, p, 0.0)
                ds = (p * (_dot(values, do, 1, 1) - delta_s[:, at])).astype(BF)
                a, g = _dot(p.astype(BF), do, 1, 0), _dot(ds, q, 1, 0)
                dv, dk = (a, g) if dv is None else (dv + a, dk + g)
                mix_s[:HEAD, at] += _dot(keys_t, ds, 1, 0)
            dv32[here, :] += dv
            dk32[here, :] += dk

        lax.fori_loop(0, b, lambda j, _: pair(j, False), None)
        pair(b, True)
        out = (mix_s[:HEAD, : heads * n] * scale).T
        cs, sn = cos_s[rows, :], sin_s[rows, :]
        for h in range(heads):
            g = out[h * n : (h + 1) * n]
            dq_s[rows, h * HEAD : (h + 1) * HEAD] = (g * cs - pltpu.roll(g, HEAD // 2, 1) * sn).astype(BF)

    def keys_done(b):
        rows = pl.ds(al(b * R, R), R)
        g = dk32[rows, :] * scale
        dkv_s[rows, :HEAD] = (g * cos_s[rows, :] - pltpu.roll(g, HEAD // 2, 1) * sin_s[rows, :]).astype(BF)
        dkv_s[rows, HEAD:] = dv32[rows, :].astype(BF)

    def term(b, k):
        rows, at = pl.ds(al(b * R, R), R), pl.ds(al(k * half, half), half)
        return _dot(dq_s[rows, :], wq_s[at, :], 1, 1) + _dot(dkv_s[rows, :], wkv_s[at, :], 1, 1)

    def dy_copy(i, b):
        return pltpu.make_async_copy(dy_s.at[pl.ds(al(2 * R + (1 - i) * R, R), R)], dy_out.at[pl.ds(al(b * R, R), R)], loc.at[L_Y0 + i])

    def give_hi(k):
        return remote(a_s.at[pl.ds(0, R), pl.ds(al(k * half, half), half)], recv_s.at[k], HD + k, partner, False)

    def hi_copy(k):
        return remote(a_s.at[pl.ds(0, R), pl.ds(al(k * half, half), half)], hi_out.at[k], HI + k, across, False)

    def add_up(k, got, x, scales, first, give=None):
        s = scales[pl.ds(al(first, R), R), :]
        for at in range(0, half, HEAD):
            col = pl.ds(al(k * half + at, HEAD), HEAD)
            v = stage[k, :, at : at + HEAD] + got(at, col).astype(F32)
            if give is None:
                stage[k, :, at : at + HEAD] = v
            else:
                a_s[give, col] = v.astype(BF)
            v = v * (x[:, col].astype(F32) * s)
            sum_s[:, col] += sum(v[r : r + 8] for r in range(0, R, 8))

    far_hi, far_lo = (1 - chip) * 2 + 1, (1 - chip) * 2

    def pass_on(i):
        dy_ici[i].wait_recv()
        remote(dy_s.at[y_far(i, c)], dy_s.at[y_far(i, c)], G0 + i, partner)

    def piece(i, b):
        first, n = PIECES[i]
        remote(dy_s.at[y_far(i, 1 - c)], dy_s.at[y_far(i, 1 - c)], G0 + i, partner, False).wait_recv()
        do_s[pl.ds(al(b * R + first % R, n), n), :] = _dot(wo_s[...], dy_s[pl.ds(2 * R + first, n), :], 1, 1).T.astype(BF)

    own_x = pltpu.make_async_copy(x_hbm, a_s.at[pl.ds(3 * R, R)], loc.at[L_X])

    def backward_step(s, _):
        @pl.when(s == 1)
        def _():
            pass_on(0)

        @pl.when(s == 2)
        def _():
            for k in range(4):
                for n in range(2):
                    a_copy(k, n).wait()
            c_gain.wait()
            own_x.start()
            piece(0, far_hi)
            dy_copy(0, far_hi).start()

        backward_block(jnp.where(s < 2, chip * 2 + 1 - s, far_hi))

        @pl.when(s == 2)
        def _():
            pass_on(1)
            keys_done(far_hi)

            def hi_part(k, _):
                @pl.when(c == 0)
                def _():
                    a_s[pl.ds(0, R), pl.ds(al(k * half, half), half)] = term(far_hi, k).astype(BF)
                    give_hi(k).start()

                @pl.when(c == 1)
                def _():
                    stage[k] = term(far_hi, k)

            lax.fori_loop(0, 2, hi_part, None)

            def hi_sum(k, _):
                give_hi(k).wait_recv()
                add_up(k, lambda at, col: recv_s[k, :, at : at + HEAD], far_x, far_scale, 0, pl.ds(0, R))
                hi_copy(k).start()

            @pl.when(c == 1)
            def _():
                lax.fori_loop(0, 2, hi_sum, None)

    lax.fori_loop(0, 3, backward_step, None)
    piece(1, far_lo)

    @pl.when(c == 1)
    def _():
        pass_on(2)

    backward_block(far_lo, Q)

    @pl.when(c == 0)
    def _():
        pass_on(2)

    piece(2, far_lo)
    dy_copy(1, far_lo).start()
    backward_block(far_lo, 0)
    keys_done(far_lo)
    c_dq = local(dq_s, dq_out, L_DQ)
    keys_done(chip * 2)
    keys_done(chip * 2 + 1)
    c_dkv = local(dkv_s, dkv_out, L_DKV)

    def place(i, k):
        return pl.ds(al(R + i * R, R), R), pl.ds(al(k * half, half), half)

    def give_half(i, k):
        rows, at = place(i, k)
        return remote(a_s.at[rows, at], near_recv.at[:, at] if i == 0 else recv_s.at[k], (ND if i == 0 else LD) + k, partner, False)

    def lo_copy(k):
        rows, at = place(1, k)
        return pltpu.make_async_copy(a_s.at[rows, at], lo_out.at[:, at], loc.at[L_LO + k])

    def near_copy(k):
        return pltpu.make_async_copy(stage.at[k], near_out.at[:, pl.ds(al(k * half, half), half)], loc.at[L_NEAR + k])

    def give_part(n, _):
        k, low = lax.rem(n, 2), lax.div(n, 2) != c
        b = jnp.where(low, (1 - chip) * 2, chip * 2 + 1 - c)

        @pl.when(low & (c == 0))
        def _():
            rows, at = place(1, k)
            stage[k] = term(b, k)
            give_half(1, k).wait_recv()
            add_up(k, lambda at, col: recv_s[k, :, at : at + HEAD], far_x, far_scale, 0, rows)
            lo_copy(k).start()

        @pl.when(jnp.logical_not(low & (c == 0)))
        def _():
            rows, at = place(jnp.where(low, 1, 0), k)
            a_s[rows, at] = term(b, k).astype(BF)

            @pl.when(low)
            def _():
                give_half(1, k).start()

            @pl.when(jnp.logical_not(low))
            def _():
                give_half(0, k).start()

    lax.fori_loop(0, 4, give_part, None)

    own_x.wait()

    def own_part(k, _):
        stage[k] = term(chip * 2 + c, k)
        give_half(0, k).wait_recv()
        add_up(k, lambda at, col: near_recv[:, col], a_s.at[pl.ds(3 * R, R)], scale_s, c * R)
        near_copy(k).start()

    lax.fori_loop(0, 2, own_part, None)
    part_s[...] = sum_s[...].sum(axis=0, keepdims=True)
    gives = [remote(part_s, parts_out.at[k], GD + k, peer) for k, peer in enumerate((partner, across, (1 - chip) * 2 + 1 - c))]
    c_part = local(part_s, parts_out.at[3], L_X)
    c_scale = local(scale_s.at[pl.ds(al(c * R, R), R)], scale_out, L_G)

    @pl.when(c == 1)
    def _():
        for k in range(2):
            hi_copy(k).wait()
            give_half(1, k).wait_send()

    @pl.when(c == 0)
    def _():
        for k in range(2):
            lo_copy(k).wait()
            give_hi(k).wait_send()

    for i in range(3):
        remote(dy_s.at[y_far(i, c)], dy_s.at[y_far(i, c)], G0 + i, partner, False).wait_send()
    for i in range(2):
        dy_copy(i, far_hi if i == 0 else far_lo).wait()
        give_half(0, i).wait_send()
        near_copy(i).wait()
    for copy in gives:
        copy.wait()
    for copy in sends:
        copy.wait_send()
    for copy in (c_o, c_yn, c_dq, c_dkv, c_scale, c_part):
        copy.wait()


def main(x, dy, gain, wq, wk, wv, wo):
    R, d = x.shape
    n, width = 4 * R, wq.shape[1]
    heads = width // HEAD
    table = jnp.asarray(np.stack(tables(n)))
    any_ = pl.BlockSpec(memory_space=pl.ANY)
    vm = pltpu.VMEM
    flops = 2 * n * d * (3 * width + 4 * HEAD) + 7 * n * n * width
    return pl.pallas_call(
        main_kernel,
        in_specs=[any_] * 8,
        out_specs=[any_] * 11,
        out_shape=[jax.ShapeDtypeStruct((n, d), BF), jax.ShapeDtypeStruct((n, d), BF), jax.ShapeDtypeStruct((n, width), BF), jax.ShapeDtypeStruct((n, width), BF),
                   jax.ShapeDtypeStruct((n, 2 * HEAD), BF), jax.ShapeDtypeStruct((R, d), F32), jax.ShapeDtypeStruct((2, R, d // 2), BF), jax.ShapeDtypeStruct((R, d), BF), jax.ShapeDtypeStruct((1, d), F32), jax.ShapeDtypeStruct((R, HEAD), F32), jax.ShapeDtypeStruct((4, 1, d), F32)],
        scratch_shapes=[vm((n, d), BF), vm((n, d), BF), vm((d,), BF), vm((1, d), F32), vm(table.shape, F32), vm((n, HEAD), F32), vm((n, HEAD), F32), vm((d, width), BF), vm((d, 2 * HEAD), BF), vm((width, d), BF),
                        vm((n, width), BF), vm((n, HEAD), BF), vm((n, HEAD), BF), vm((n, width), BF), vm((n, width), BF), vm((n, width), BF),
                        vm((n, HEAD), F32), vm((n, HEAD), F32), vm((n, 2 * HEAD), BF), vm((4, 1, heads * R), F32), vm((1, heads * R), F32), vm((1, heads * R), F32), vm((HEAD + 8, heads * R), F32),
                        vm((2, R, d // 2), BF), vm((R, d), BF), vm((2, R, d // 2), F32),
                        vm((R, d), BF), vm((2 * R, HEAD), F32), vm((R, HEAD), F32), vm((8, d), F32), vm((1, d), F32),
                        pltpu.SemaphoreType.DMA((N_LOCAL,)), pltpu.SemaphoreType.DMA((N_REMOTE,)), pltpu.SemaphoreType.DMA((N_REMOTE,))],
        compiler_params=pltpu.CompilerParams(collective_id=0, has_side_effects=True, vmem_limit_bytes=67043328),
        cost_estimate=pl.CostEstimate(flops=flops, bytes_accessed=60 * 2**20, transcendentals=n * n * heads),
        name="main",
    )(x, dy, gain, table, wq, wk, wv, wo)


def row_scale(x):
    return lax.rsqrt(jnp.mean(x * x, -1, keepdims=True) + 1e-6)


def weights_kernel(a_ref, dq_ref, dkv_ref, o_ref, dy_ref, wq_ref, wk_ref, wv_ref, wo_ref):
    a = a_ref[...]
    wq_ref[...] = _dot(a, dq_ref[...], 0, 0).astype(BF)
    kv = _dot(a, dkv_ref[...], 0, 0).astype(BF)
    wk_ref[...] = kv[:, :HEAD]
    wv_ref[...] = kv[:, HEAD:]
    wo_ref[...] = _dot(o_ref[...], dy_ref[...], 0, 0).astype(BF)


def weight_gradients(a, dq, dkv, o, dy, tile=512):
    n, d = a.shape
    width = dq.shape[1]
    tall = pl.BlockSpec((n, tile), lambda i: (0, i))
    whole = lambda w: pl.BlockSpec((n, w), lambda i: (0, 0))
    rows = lambda w: pl.BlockSpec((tile, w), lambda i: (i, 0))
    return pl.pallas_call(
        weights_kernel,
        grid=(d // tile,),
        in_specs=[tall, whole(width), whole(2 * HEAD), whole(width), tall],
        out_specs=[rows(width), rows(HEAD), rows(HEAD), pl.BlockSpec((width, tile), lambda i: (0, i))],
        out_shape=[jax.ShapeDtypeStruct((d, width), BF), jax.ShapeDtypeStruct((d, HEAD), BF), jax.ShapeDtypeStruct((d, HEAD), BF), jax.ShapeDtypeStruct((width, d), BF)],
        compiler_params=pltpu.CompilerParams(dimension_semantics=("arbitrary",), vmem_limit_bytes=62 * 2**20),
        cost_estimate=pl.CostEstimate(flops=2 * n * d * (2 * width + 2 * HEAD), bytes_accessed=2 * (2 * n * d + 2 * n * width + 2 * d * width), transcendentals=0),
        name="weights",
    )(a, dq, dkv, o, dy)


def close_kernel(chunk, x_hbm, dy_hbm, near_hbm, hi_hbm, lo_hbm, gain_hbm, scale_hbm, parts_hbm, dx_hbm, dgain_hbm, x_s, dy_s, near_s, far_s, dx_s, gain_s, scale_s, parts_s, dgain_s, in_sem, out_sem):
    R, d = x_s.shape
    half = d // 2
    upper = lax.rem(lax.axis_index("tp"), 2) == 1
    n = R // chunk

    def loads(i):
        r = pl.ds(i * chunk, chunk)
        return [pltpu.make_async_copy(src.at[r], dst.at[r], in_sem.at[i, k]) for k, (src, dst) in enumerate(((x_hbm, x_s), (near_hbm, near_s), (dy_hbm, dy_s)))]

    def high(i, k):
        r = pl.ds(i * chunk, chunk)
        return pltpu.make_async_copy(hi_hbm.at[k, r], far_s.at[r, pl.ds(k * half, half)], in_sem.at[i, 3 + k])

    def low(i):
        r = pl.ds(i * chunk, chunk)
        return pltpu.make_async_copy(lo_hbm.at[r], far_s.at[r], in_sem.at[i, 3])

    def fars(act):
        @pl.when(upper)
        def _():
            for k in range(2):
                act(lambda i: high(i, k))

        @pl.when(jnp.logical_not(upper))
        def _():
            act(low)

    small = [pltpu.make_async_copy(src, dst, out_sem.at[n + k]) for k, (src, dst) in enumerate(((gain_hbm, gain_s), (scale_hbm, scale_s), (parts_hbm, parts_s)))]
    for copy in small:
        copy.start()
    for i in range(n):
        for copy in loads(i):
            copy.start()
        fars(lambda make: make(i).start())

    def store(i):
        r = pl.ds(i * chunk, chunk)
        return pltpu.make_async_copy(dx_s.at[r], dx_hbm.at[r], out_sem.at[i])

    columns = [slice(at, at + HEAD) for at in range(0, d, HEAD)]
    for copy in small:
        copy.wait()
    dgain_s[...] = (parts_s[3] + parts_s[0]) + (parts_s[1] + parts_s[2])
    give_gain = pltpu.make_async_copy(dgain_s, dgain_hbm, out_sem.at[n])
    give_gain.start()
    for i in range(n):
        for copy in loads(i):
            copy.wait()
        fars(lambda make: make(i).wait())
        r = slice(i * chunk, (i + 1) * chunk)
        s = scale_s[r, :]
        dot = jnp.zeros((chunk, HEAD), F32)
        for at in columns:
            g = (near_s[r, at] + far_s[r, at].astype(F32)) * gain_s[:, at]
            near_s[r, at] = g
            dot += g * x_s[r, at].astype(F32)
        m = s * s * s * (dot.sum(-1, keepdims=True) * (1 / d))
        for at in columns:
            dx_s[r, at] = (dy_s[r, at].astype(F32) + near_s[r, at] * s - x_s[r, at].astype(F32) * m).astype(BF)
        store(i).start()
    give_gain.wait()
    for i in range(n):
        store(i).wait()


def close(x, dy, near, hi, lo, gain, scale, parts, chunk=64):
    R, d = x.shape
    hbm = pl.BlockSpec(memory_space=pltpu.HBM)
    vm = pltpu.VMEM
    return pl.pallas_call(
        functools.partial(close_kernel, chunk),
        in_specs=[hbm] * 8,
        out_specs=[hbm] * 2,
        out_shape=[jax.ShapeDtypeStruct((R, d), BF), jax.ShapeDtypeStruct((1, d), F32)],
        scratch_shapes=[vm((R, d), BF), vm((R, d), BF), vm((R, d), F32), vm((R, d), BF), vm((R, d), BF), vm((1, d), F32), vm((R, HEAD), F32), vm((4, 1, d), F32), vm((1, d), F32),
                        pltpu.SemaphoreType.DMA((R // chunk, 5)), pltpu.SemaphoreType.DMA((R // chunk + 3,))],
        compiler_params=pltpu.CompilerParams(vmem_limit_bytes=62 * 2**20),
        cost_estimate=pl.CostEstimate(flops=16 * R * d, bytes_accessed=12 * R * d, transcendentals=R),
        name="close",
    )(x, dy, near, hi, lo, gain, scale, parts)


def solution(mesh):
    def step(x, dy, gain, wq, wk, wv, wo):
        a, dy_all, o, dq, dkv, near, hi, lo, gain_row, scale, parts = main(x, dy, gain, wq, wk, wv, wo)
        got = lax.ppermute(lo, "tp", [(0, 2), (2, 0)])
        by_wq, by_wk, by_wv, by_wo = weight_gradients(a, dq, dkv, o, dy_all)
        gain_row, by_wk = lax.optimization_barrier((gain_row, by_wk))
        by_x, by_gain = close(x, dy, near, hi, got, gain_row, scale, parts)
        return by_x, by_gain, by_wq, by_wk, by_wv, by_wo

    tokens, columns = P(("dp", "tp"), None), P(None, "tp")
    return jax.shard_map(
        step,
        mesh=mesh,
        in_specs=(tokens, tokens, P(None), columns, columns, columns, P("tp", None)),
        out_specs=(tokens, P("dp", None), P("dp", "tp"), P("dp", "tp"), P("dp", "tp"), P(("dp", "tp"), None)),
        check_vma=False,
    )
```

```python
import functools

import jax
import jax.numpy as jnp
from jax import lax
from jax.experimental import pallas as pl
from jax.experimental.pallas import tpu as pltpu

NEG = -1e30
HIDDEN = 2 * NEG
LOG2E = 1.4426950408889634
VMEM = 56 * 2**20


def _dot(a, b, ca, cb):
    return lax.dot_general(a, b, (((ca,), (cb,)), ((), ())), preferred_element_type=jnp.float32)


from jax.sharding import PartitionSpec as P
import numpy as np

HEAD = 128
THETA = 10000
MESH = pl.DeviceIdType.MESH
F32, BF = jnp.float32, jnp.bfloat16

X0, F0, XD, YD, Y0, G0, HD, LD, ND, HI, GD = 0, 2, 4, 5, 6, 9, 12, 14, 16, 18, 20
N_REMOTE = 23
L_X, L_DY, L_G, L_COS, L_WQ, L_WK, L_WV, L_WO, L_YN, L_A0, L_Y0, L_O, L_DQ, L_DKV, L_LO, L_NEAR = 0, 1, 2, 3, 4, 5, 6, 7, 8, 9, 17, 19, 20, 21, 22, 24
N_LOCAL = 26
FINE = 32


def tables(rows):
    half = HEAD // 2
    rate = float(THETA) ** (-np.arange(half, dtype=np.float64) / half)
    place = np.concatenate([np.arange(0, rows, FINE), np.arange(FINE)]).astype(np.float64)
    angle = place[:, None] * np.concatenate([rate, rate])[None]
    return np.cos(angle).astype(np.float32), np.sin(angle).astype(np.float32)


def main_kernel(x_hbm, dy_hbm, gain_hbm, table_hbm, wq_hbm, wk_hbm, wv_hbm, wo_hbm,
                a_out, dy_out, o_out, dq_out, dkv_out, near_out, hi_out, lo_out, gain_out, scale_out, parts_out,
                a_s, dy_s, gain_1, gain_s, table_s, cos_s, sin_s, wq_s, wkv_s, wo_s, q_s, k_s, v_s, o_s, do_s, dq_s, dk32, dv32, dkv_s, lse_s, delta_s, top_s, mix_s,
                recv_s, near_recv, stage, far_x, scale_s, far_scale, sum_s, part_s, loc, snd, rcv):
    t = lax.axis_index("tp")
    chip, c = lax.div(t, 2), lax.rem(t, 2)
    partner, across = chip * 2 + 1 - c, (1 - chip) * 2 + c
    d = a_s.shape[1]
    half = d // 2
    R = x_hbm.shape[0]
    Q = R // 2
    heads = wq_hbm.shape[1] // HEAD
    cols = heads * R
    wide = 2 * R
    scale = HEAD**-0.5
    e = scale * LOG2E
    al = pl.multiple_of

    def local(src, dst, i):
        copy = pltpu.make_async_copy(src, dst, loc.at[i])
        copy.start()
        return copy

    def remote(src, dst, i, device, start=True):
        copy = pltpu.make_async_remote_copy(src_ref=src, dst_ref=dst, send_sem=snd.at[i], recv_sem=rcv.at[i], device_id={"tp": device}, device_id_type=MESH)
        if start:
            copy.start()
        return copy

    own = pl.ds(al(c * R, R), R)
    theirs = pl.ds(al((1 - c) * R, R), R)
    c_x = local(x_hbm, a_s.at[own], L_X)
    c_dy = local(dy_hbm, dy_s.at[own], L_DY)
    c_g = local(gain_hbm, gain_1, L_G)

    barrier = pltpu.get_barrier_semaphore()
    for k in range(1, 4):
        pl.semaphore_signal(barrier, inc=1, device_id={"tp": lax.rem(t + k, 4)}, device_id_type=MESH)
    pl.semaphore_wait(barrier, 3)

    def x_at(i, k):
        return pl.ds(al(2 * R + i * R + k * Q, Q), Q)

    PIECES = ((R, R), (Q, Q), (0, Q))

    def y_near(i, k):
        first, n = PIECES[i]
        return pl.ds(al(first + k * (n // 2), n // 2), n // 2)

    def y_far(i, k):
        first, n = PIECES[i]
        return pl.ds(al(2 * R + first + k * (n // 2), n // 2), n // 2)

    sends = []
    sends += [remote(x_hbm.at[pl.ds(i * Q, Q)], far_x.at[pl.ds(i * Q, Q)], X0 + i, across) for i in range(2)]
    sends += [remote(x_hbm, a_s.at[own], XD, partner), remote(dy_hbm, dy_s.at[own], YD, partner)]
    c_table = local(table_hbm, table_s, L_COS)
    c_wq = local(wq_hbm, wq_s, L_WQ)
    c_wk, c_wv = local(wk_hbm, wkv_s.at[:, pl.ds(0, HEAD)], L_WK), local(wv_hbm, wkv_s.at[:, pl.ds(HEAD, HEAD)], L_WV)
    c_wo = local(wo_hbm, wo_s, L_WO)

    def normed_rows(src, first, start, n, kept=None, place=0):
        def body(i, _):
            x = src[pl.ds(al(first + i * 16, 16), 16), :].astype(F32)
            s = lax.rsqrt(jnp.mean(x * x, -1, keepdims=True) + 1e-6)
            a_s[pl.ds(al(start + i * 16, 16), 16), :] = (x * s * gain_s[...]).astype(BF)
            if kept is not None:
                kept[pl.ds(al(place + i * 16, 16), 16), :] = jnp.broadcast_to(s, (16, HEAD))

        lax.fori_loop(0, n // 16, body, None)

    def turn(ref, n_heads, start, n):
        def body(i, _):
            r = pl.ds(al(start + i * 32, 32), 32)
            cs, sn = cos_s[r, :], sin_s[r, :]
            for h in range(n_heads):
                at = slice(h * HEAD, (h + 1) * HEAD)
                v = ref[r, at].astype(F32)
                ref[r, at] = (v * cs + pltpu.roll(v, HEAD // 2, 1) * sn).astype(BF)

        lax.fori_loop(0, n // 32, body, None)

    near0, far0 = chip * 2 * R, (1 - chip) * 2 * R

    c_dy.wait()
    remote(dy_hbm, dy_s.at[theirs], YD, partner, False).wait_recv()
    dy_ici = [remote(dy_s.at[y_near(i, c)], dy_s.at[y_far(i, c)], Y0 + i, across) for i in range(3)]
    sends += dy_ici
    c_g.wait()
    gain_s[...] = gain_1[...].astype(F32).reshape(1, d)
    c_table.wait()
    c_gain = local(gain_s, gain_out, L_COS)
    few = cos_s.shape[0] // FINE
    side = jnp.where(lax.broadcasted_iota(jnp.int32, (1, HEAD), 1) < HEAD // 2, -1.0, 1.0)

    def angles(i, _):
        r = pl.ds(al(i * FINE, FINE), FINE)
        ca, sa = table_s[0, pl.ds(i, 1), :], table_s[1, pl.ds(i, 1), :]
        cb, sb = table_s[0, few:, :], table_s[1, few:, :]
        cos_s[r, :] = ca * cb - sa * sb
        sin_s[r, :] = (sa * cb + ca * sb) * side

    lax.fori_loop(0, few, angles, None)
    c_x.wait()
    remote(x_hbm, a_s.at[theirs], XD, partner, False).wait_recv()

    def a_copy(i, k):
        token = jnp.where(i < 2, near0 + i * R + k * Q, far0 + (i - 2) * Q + k * R)
        return pltpu.make_async_copy(a_s.at[pl.ds(al(i * R + k * Q, Q), Q)], a_out.at[pl.ds(al(token, Q), Q)], loc.at[L_A0 + 2 * i + k])

    def project_block(i, _):
        @pl.when(i >= 2)
        def _():
            j = i - 2
            landed = far_x.at[pl.ds(al(j * Q, Q), Q)]
            remote(x_hbm.at[pl.ds(0, Q)], landed, X0 + j, across, False).wait_recv()
            give = remote(landed, a_s.at[x_at(j, c)], F0 + j, partner)
            normed_rows(far_x, j * Q, 2 * R + j * R + c * Q, Q, far_scale, j * Q)
            remote(landed, a_s.at[x_at(j, 1 - c)], F0 + j, partner, False).wait_recv()
            normed_rows(a_s, 2 * R + j * R + (1 - c) * Q, 2 * R + j * R + (1 - c) * Q, Q)
            give.wait_send()

        @pl.when(i < 2)
        def _():
            normed_rows(a_s, i * R, i * R, R, scale_s, i * R)

        for k in range(2):
            a_copy(i, k).start()

        @pl.when(i == 0)
        def _():
            for w in (c_wq, c_wk, c_wv):
                w.wait()

        block = pl.ds(al(i * R, R), R)
        r = _dot(a_s[block, :], wq_s[...], 1, 0).astype(BF)
        kv = _dot(a_s[block, :], wkv_s[...], 1, 0).astype(BF)
        for k in range(2):
            token = jnp.where(i < 2, near0 + i * R + k * Q, far0 + (i - 2) * Q + k * R)
            p = pl.ds(al(token, Q), Q)
            q_s[p, :] = r[k * Q : (k + 1) * Q]
            k_s[p, :] = kv[k * Q : (k + 1) * Q, :HEAD]
            v_s[p, :] = kv[k * Q : (k + 1) * Q, HEAD:]
            turn(q_s, heads, token, Q)
            turn(k_s, 1, token, Q)

        @pl.when(i < 2)
        def _():
            @pl.when(i == 0)
            def _():
                c_wo.wait()

            do_s[pl.ds(al(near0 + i * R, R), R), :] = _dot(dy_s[block, :], wo_s[...], 1, 1).astype(BF)

    sum_s[...] = jnp.zeros_like(sum_s)
    dk32[...] = jnp.zeros_like(dk32)
    dv32[...] = jnp.zeros_like(dv32)
    lax.fori_loop(0, 4, project_block, None)
    c_yn = local(dy_s.at[pl.ds(0, 2 * R)], dy_out.at[pl.ds(al(near0, 2 * R), 2 * R)], L_YN)

    def seen_mask():
        return lax.rem(lax.broadcasted_iota(jnp.int32, (R, wide), 1), R) >= lax.broadcasted_iota(jnp.int32, (R, wide), 0)

    strips = range(0, cols, wide)

    def strip(ref, rows, at):
        h = at // R
        return jnp.concatenate([ref[rows, (h + n) * HEAD : (h + n + 1) * HEAD] for n in range(wide // R)], axis=0)

    def attend_block(b, _):
        rows = pl.ds(al(b * R, R), R)
        top_s[...] = jnp.full(top_s.shape, NEG, F32)
        mix_s[...] = jnp.zeros_like(mix_s)

        def pair(j, masked):
            here = pl.ds(al(j * R, R), R)
            keys = k_s[here, :]
            values = jnp.concatenate([v_s[here, :].T, jnp.ones((8, R), BF)], axis=0)
            scores = [_dot(keys, strip(q_s, rows, at), 1, 1) for at in strips]
            weights, keeps = [], []
            for at, s in zip(strips, scores):
                if masked:
                    s = jnp.where(seen_mask(), s, HIDDEN)
                old = top_s[:, at : at + wide]
                top = jnp.maximum(old, s.max(axis=0, keepdims=True))
                top_s[:, at : at + wide] = top
                weights.append(jnp.exp2((s - top) * e).astype(BF))
                keeps.append(jnp.exp2((old - top) * e))
            for at, p, keep in zip(strips, weights, keeps):
                mix_s[:, at : at + wide] = mix_s[:, at : at + wide] * keep + _dot(values, p, 1, 0)

        lax.fori_loop(0, b, lambda j, _: pair(j, False), None)
        pair(b, True)
        total = mix_s[HEAD : HEAD + 1, :]
        out = (mix_s[:HEAD, :] * (1 / total)).T.astype(BF)
        for h in range(heads):
            o_s[rows, h * HEAD : (h + 1) * HEAD] = out[h * R : (h + 1) * R]
        lse_s[b] = top_s[...] * scale + jnp.log(total)

    lax.fori_loop(0, 4, attend_block, None)
    c_o = local(o_s, o_out, L_O)

    def backward_block(b, first=None):
        n, first = (R, 0) if first is None else (Q, first)
        rows = pl.ds(al(b * R + first, n), n)
        per = wide // n
        parts = [(h, slice(h * n, h * n + wide)) for h in range(0, heads, per)]

        def of(ref, h):
            return jnp.concatenate([ref[rows, (h + m) * HEAD : (h + m + 1) * HEAD] for m in range(per)], axis=0)

        for h, at in parts:
            both = of(do_s, h).astype(F32) * of(o_s, h).astype(F32)
            delta_s[:, at] = both.T.sum(axis=0, keepdims=True)
            top_s[:, at] = jnp.concatenate([lse_s[b, :, (h + m) * R + first : (h + m) * R + first + n] for m in range(per)], axis=1) * LOG2E
        mix_s[...] = jnp.zeros_like(mix_s)

        def pair(j, masked):
            here = pl.ds(al(j * R, R), R)
            keys, values = k_s[here, :], v_s[here, :]
            keys_t = keys.T
            dv = dk = None
            for h, at in parts:
                q, do = of(q_s, h), of(do_s, h)
                p = jnp.exp2(_dot(keys, q, 1, 1) * e - top_s[:, at])
                if masked:
                    seen = lax.rem(lax.broadcasted_iota(jnp.int32, (R, wide), 1), n) + first >= lax.broadcasted_iota(jnp.int32, (R, wide), 0)
                    p = jnp.where(seen, p, 0.0)
                ds = (p * (_dot(values, do, 1, 1) - delta_s[:, at])).astype(BF)
                a, g = _dot(p.astype(BF), do, 1, 0), _dot(ds, q, 1, 0)
                dv, dk = (a, g) if dv is None else (dv + a, dk + g)
                mix_s[:HEAD, at] += _dot(keys_t, ds, 1, 0)
            dv32[here, :] += dv
            dk32[here, :] += dk

        lax.fori_loop(0, b, lambda j, _: pair(j, False), None)
        pair(b, True)
        out = (mix_s[:HEAD, : heads * n] * scale).T
        cs, sn = cos_s[rows, :], sin_s[rows, :]
        for h in range(heads):
            g = out[h * n : (h + 1) * n]
            dq_s[rows, h * HEAD : (h + 1) * HEAD] = (g * cs - pltpu.roll(g, HEAD // 2, 1) * sn).astype(BF)

    def keys_done(b):
        rows = pl.ds(al(b * R, R), R)
        g = dk32[rows, :] * scale
        dkv_s[rows, :HEAD] = (g * cos_s[rows, :] - pltpu.roll(g, HEAD // 2, 1) * sin_s[rows, :]).astype(BF)
        dkv_s[rows, HEAD:] = dv32[rows, :].astype(BF)

    def term(b, k):
        rows, at = pl.ds(al(b * R, R), R), pl.ds(al(k * half, half), half)
        return _dot(dq_s[rows, :], wq_s[at, :], 1, 1) + _dot(dkv_s[rows, :], wkv_s[at, :], 1, 1)

    def dy_copy(i, b):
        return pltpu.make_async_copy(dy_s.at[pl.ds(al(2 * R + (1 - i) * R, R), R)], dy_out.at[pl.ds(al(b * R, R), R)], loc.at[L_Y0 + i])

    def give_hi(k):
        return remote(a_s.at[pl.ds(0, R), pl.ds(al(k * half, half), half)], recv_s.at[k], HD + k, partner, False)

    def hi_copy(k):
        return remote(a_s.at[pl.ds(0, R), pl.ds(al(k * half, half), half)], hi_out.at[k], HI + k, across, False)

    def add_up(k, got, x, scales, first, give=None):
        s = scales[pl.ds(al(first, R), R), :]
        for at in range(0, half, HEAD):
            col = pl.ds(al(k * half + at, HEAD), HEAD)
            v = stage[k, :, at : at + HEAD] + got(at, col).astype(F32)
            if give is None:
                stage[k, :, at : at + HEAD] = v
            else:
                a_s[give, col] = v.astype(BF)
            v = v * (x[:, col].astype(F32) * s)
            sum_s[:, col] += sum(v[r : r + 8] for r in range(0, R, 8))

    far_hi, far_lo = (1 - chip) * 2 + 1, (1 - chip) * 2

    def pass_on(i):
        dy_ici[i].wait_recv()
        remote(dy_s.at[y_far(i, c)], dy_s.at[y_far(i, c)], G0 + i, partner)

    def piece(i, b):
        first, n = PIECES[i]
        remote(dy_s.at[y_far(i, 1 - c)], dy_s.at[y_far(i, 1 - c)], G0 + i, partner, False).wait_recv()
        do_s[pl.ds(al(b * R + first % R, n), n), :] = _dot(wo_s[...], dy_s[pl.ds(2 * R + first, n), :], 1, 1).T.astype(BF)

    own_x = pltpu.make_async_copy(x_hbm, a_s.at[pl.ds(3 * R, R)], loc.at[L_X])

    def backward_step(s, _):
        @pl.when(s == 1)
        def _():
            pass_on(0)

        @pl.when(s == 2)
        def _():
            for k in range(4):
                for n in range(2):
                    a_copy(k, n).wait()
            c_gain.wait()
            own_x.start()
            piece(0, far_hi)
            dy_copy(0, far_hi).start()

        backward_block(jnp.where(s < 2, chip * 2 + 1 - s, far_hi))

        @pl.when(s == 2)
        def _():
            pass_on(1)
            keys_done(far_hi)

            def hi_part(k, _):
                @pl.when(c == 0)
                def _():
                    a_s[pl.ds(0, R), pl.ds(al(k * half, half), half)] = term(far_hi, k).astype(BF)
                    give_hi(k).start()

                @pl.when(c == 1)
                def _():
                    stage[k] = term(far_hi, k)

            lax.fori_loop(0, 2, hi_part, None)

            def hi_sum(k, _):
                give_hi(k).wait_recv()
                add_up(k, lambda at, col: recv_s[k, :, at : at + HEAD], far_x, far_scale, 0, pl.ds(0, R))
                hi_copy(k).start()

            @pl.when(c == 1)
            def _():
                lax.fori_loop(0, 2, hi_sum, None)

    lax.fori_loop(0, 3, backward_step, None)
    piece(1, far_lo)

    @pl.when(c == 1)
    def _():
        pass_on(2)

    backward_block(far_lo, Q)

    @pl.when(c == 0)
    def _():
        pass_on(2)

    piece(2, far_lo)
    dy_copy(1, far_lo).start()
    backward_block(far_lo, 0)
    keys_done(far_lo)
    c_dq = local(dq_s, dq_out, L_DQ)
    keys_done(chip * 2)
    keys_done(chip * 2 + 1)
    c_dkv = local(dkv_s, dkv_out, L_DKV)

    def place(i, k):
        return pl.ds(al(R + i * R, R), R), pl.ds(al(k * half, half), half)

    def give_half(i, k):
        rows, at = place(i, k)
        return remote(a_s.at[rows, at], near_recv.at[:, at] if i == 0 else recv_s.at[k], (ND if i == 0 else LD) + k, partner, False)

    def lo_copy(k):
        rows, at = place(1, k)
        return pltpu.make_async_copy(a_s.at[rows, at], lo_out.at[:, at], loc.at[L_LO + k])

    def near_copy(k):
        return pltpu.make_async_copy(stage.at[k], near_out.at[:, pl.ds(al(k * half, half), half)], loc.at[L_NEAR + k])

    def give_part(n, _):
        k, low = lax.rem(n, 2), lax.div(n, 2) != c
        b = jnp.where(low, (1 - chip) * 2, chip * 2 + 1 - c)

        @pl.when(low & (c == 0))
        def _():
            rows, at = place(1, k)
            stage[k] = term(b, k)
            give_half(1, k).wait_recv()
            add_up(k, lambda at, col: recv_s[k, :, at : at + HEAD], far_x, far_scale, 0, rows)
            lo_copy(k).start()

        @pl.when(jnp.logical_not(low & (c == 0)))
        def _():
            rows, at = place(jnp.where(low, 1, 0), k)
            a_s[rows, at] = term(b, k).astype(BF)

            @pl.when(low)
            def _():
                give_half(1, k).start()

            @pl.when(jnp.logical_not(low))
            def _():
                give_half(0, k).start()

    lax.fori_loop(0, 4, give_part, None)

    own_x.wait()

    def own_part(k, _):
        stage[k] = term(chip * 2 + c, k)
        give_half(0, k).wait_recv()
        add_up(k, lambda at, col: near_recv[:, col], a_s.at[pl.ds(3 * R, R)], scale_s, c * R)
        near_copy(k).start()

    lax.fori_loop(0, 2, own_part, None)
    part_s[...] = sum_s[...].sum(axis=0, keepdims=True)
    gives = [remote(part_s, parts_out.at[k], GD + k, peer) for k, peer in enumerate((partner, across, (1 - chip) * 2 + 1 - c))]
    c_part = local(part_s, parts_out.at[3], L_X)
    c_scale = local(scale_s.at[pl.ds(al(c * R, R), R)], scale_out, L_G)

    @pl.when(c == 1)
    def _():
        for k in range(2):
            hi_copy(k).wait()
            give_half(1, k).wait_send()

    @pl.when(c == 0)
    def _():
        for k in range(2):
            lo_copy(k).wait()
            give_hi(k).wait_send()

    for i in range(3):
        remote(dy_s.at[y_far(i, c)], dy_s.at[y_far(i, c)], G0 + i, partner, False).wait_send()
    for i in range(2):
        dy_copy(i, far_hi if i == 0 else far_lo).wait()
        give_half(0, i).wait_send()
        near_copy(i).wait()
    for copy in gives:
        copy.wait()
    for copy in sends:
        copy.wait_send()
    for copy in (c_o, c_yn, c_dq, c_dkv, c_scale, c_part):
        copy.wait()


def main(x, dy, gain, wq, wk, wv, wo):
    R, d = x.shape
    n, width = 4 * R, wq.shape[1]
    heads = width // HEAD
    table = jnp.asarray(np.stack(tables(n)))
    any_ = pl.BlockSpec(memory_space=pl.ANY)
    vm = pltpu.VMEM
    flops = 2 * n * d * (3 * width + 4 * HEAD) + 7 * n * n * width
    return pl.pallas_call(
        main_kernel,
        in_specs=[any_] * 8,
        out_specs=[any_] * 11,
        out_shape=[jax.ShapeDtypeStruct((n, d), BF), jax.ShapeDtypeStruct((n, d), BF), jax.ShapeDtypeStruct((n, width), BF), jax.ShapeDtypeStruct((n, width), BF),
                   jax.ShapeDtypeStruct((n, 2 * HEAD), BF), jax.ShapeDtypeStruct((R, d), F32), jax.ShapeDtypeStruct((2, R, d // 2), BF), jax.ShapeDtypeStruct((R, d), BF), jax.ShapeDtypeStruct((1, d), F32), jax.ShapeDtypeStruct((R, HEAD), F32), jax.ShapeDtypeStruct((4, 1, d), F32)],
        scratch_shapes=[vm((n, d), BF), vm((n, d), BF), vm((d,), BF), vm((1, d), F32), vm(table.shape, F32), vm((n, HEAD), F32), vm((n, HEAD), F32), vm((d, width), BF), vm((d, 2 * HEAD), BF), vm((width, d), BF),
                        vm((n, width), BF), vm((n, HEAD), BF), vm((n, HEAD), BF), vm((n, width), BF), vm((n, width), BF), vm((n, width), BF),
                        vm((n, HEAD), F32), vm((n, HEAD), F32), vm((n, 2 * HEAD), BF), vm((4, 1, heads * R), F32), vm((1, heads * R), F32), vm((1, heads * R), F32), vm((HEAD + 8, heads * R), F32),
                        vm((2, R, d // 2), BF), vm((R, d), BF), vm((2, R, d // 2), F32),
                        vm((R, d), BF), vm((2 * R, HEAD), F32), vm((R, HEAD), F32), vm((8, d), F32), vm((1, d), F32),
                        pltpu.SemaphoreType.DMA((N_LOCAL,)), pltpu.SemaphoreType.DMA((N_REMOTE,)), pltpu.SemaphoreType.DMA((N_REMOTE,))],
        compiler_params=pltpu.CompilerParams(collective_id=0, has_side_effects=True, vmem_limit_bytes=67043328),
        cost_estimate=pl.CostEstimate(flops=flops, bytes_accessed=60 * 2**20, transcendentals=n * n * heads),
        name="main",
    )(x, dy, gain, table, wq, wk, wv, wo)


def row_scale(x):
    return lax.rsqrt(jnp.mean(x * x, -1, keepdims=True) + 1e-6)


def weights_kernel(a_ref, dq_ref, dkv_ref, o_ref, dy_ref, wq_ref, wk_ref, wv_ref, wo_ref):
    a = a_ref[...]
    width = dq_ref.shape[1]
    both = _dot(a, jnp.concatenate([dq_ref[...], dkv_ref[...]], axis=1), 0, 0).astype(BF)
    wq_ref[...] = both[:, :width]
    wk_ref[...] = both[:, width : width + HEAD]
    wv_ref[...] = both[:, width + HEAD :]
    wo_ref[...] = _dot(o_ref[...], dy_ref[...], 0, 0).astype(BF)


def weight_gradients(a, dq, dkv, o, dy, tile=512):
    n, d = a.shape
    width = dq.shape[1]
    tall = pl.BlockSpec((n, tile), lambda i: (0, i))
    whole = lambda w: pl.BlockSpec((n, w), lambda i: (0, 0))
    rows = lambda w: pl.BlockSpec((tile, w), lambda i: (i, 0))
    return pl.pallas_call(
        weights_kernel,
        grid=(d // tile,),
        in_specs=[tall, whole(width), whole(2 * HEAD), whole(width), tall],
        out_specs=[rows(width), rows(HEAD), rows(HEAD), pl.BlockSpec((width, tile), lambda i: (0, i))],
        out_shape=[jax.ShapeDtypeStruct((d, width), BF), jax.ShapeDtypeStruct((d, HEAD), BF), jax.ShapeDtypeStruct((d, HEAD), BF), jax.ShapeDtypeStruct((width, d), BF)],
        compiler_params=pltpu.CompilerParams(dimension_semantics=("arbitrary",), vmem_limit_bytes=62 * 2**20),
        cost_estimate=pl.CostEstimate(flops=2 * n * d * (2 * width + 2 * HEAD), bytes_accessed=2 * (2 * n * d + 2 * n * width + 2 * d * width), transcendentals=0),
        name="weights",
    )(a, dq, dkv, o, dy)


def close_kernel(chunk, x_hbm, dy_hbm, near_hbm, hi_hbm, lo_hbm, gain_hbm, scale_hbm, parts_hbm, dx_hbm, dgain_hbm, x_s, dy_s, near_s, far_s, dx_s, gain_s, scale_s, parts_s, dgain_s, in_sem, out_sem):
    R, d = x_s.shape
    half = d // 2
    upper = lax.rem(lax.axis_index("tp"), 2) == 1
    n = R // chunk

    def loads(i):
        r = pl.ds(i * chunk, chunk)
        return [pltpu.make_async_copy(src.at[r], dst.at[r], in_sem.at[i, k]) for k, (src, dst) in enumerate(((x_hbm, x_s), (near_hbm, near_s), (dy_hbm, dy_s)))]

    def high(i, k):
        r = pl.ds(i * chunk, chunk)
        return pltpu.make_async_copy(hi_hbm.at[k, r], far_s.at[r, pl.ds(k * half, half)], in_sem.at[i, 3 + k])

    def low(i):
        r = pl.ds(i * chunk, chunk)
        return pltpu.make_async_copy(lo_hbm.at[r], far_s.at[r], in_sem.at[i, 3])

    def fars(act):
        @pl.when(upper)
        def _():
            for k in range(2):
                act(lambda i: high(i, k))

        @pl.when(jnp.logical_not(upper))
        def _():
            act(low)

    small = [pltpu.make_async_copy(src, dst, out_sem.at[n + k]) for k, (src, dst) in enumerate(((gain_hbm, gain_s), (scale_hbm, scale_s), (parts_hbm, parts_s)))]
    for copy in small:
        copy.start()
    for i in range(n):
        for copy in loads(i):
            copy.start()
        fars(lambda make: make(i).start())

    def store(i):
        r = pl.ds(i * chunk, chunk)
        return pltpu.make_async_copy(dx_s.at[r], dx_hbm.at[r], out_sem.at[i])

    columns = [slice(at, at + HEAD) for at in range(0, d, HEAD)]
    for copy in small:
        copy.wait()
    dgain_s[...] = (parts_s[3] + parts_s[0]) + (parts_s[1] + parts_s[2])
    give_gain = pltpu.make_async_copy(dgain_s, dgain_hbm, out_sem.at[n])
    give_gain.start()
    for i in range(n):
        for copy in loads(i):
            copy.wait()
        fars(lambda make: make(i).wait())
        r = slice(i * chunk, (i + 1) * chunk)
        s = scale_s[r, :]
        dot = jnp.zeros((chunk, HEAD), F32)
        for at in columns:
            g = (near_s[r, at] + far_s[r, at].astype(F32)) * gain_s[:, at]
            near_s[r, at] = g
            dot += g * x_s[r, at].astype(F32)
        m = s * s * s * (dot.sum(-1, keepdims=True) * (1 / d))
        for at in columns:
            dx_s[r, at] = (dy_s[r, at].astype(F32) + near_s[r, at] * s - x_s[r, at].astype(F32) * m).astype(BF)
        store(i).start()
    give_gain.wait()
    for i in range(n):
        store(i).wait()


def close(x, dy, near, hi, lo, gain, scale, parts, chunk=64):
    R, d = x.shape
    hbm = pl.BlockSpec(memory_space=pltpu.HBM)
    vm = pltpu.VMEM
    return pl.pallas_call(
        functools.partial(close_kernel, chunk),
        in_specs=[hbm] * 8,
        out_specs=[hbm] * 2,
        out_shape=[jax.ShapeDtypeStruct((R, d), BF), jax.ShapeDtypeStruct((1, d), F32)],
        scratch_shapes=[vm((R, d), BF), vm((R, d), BF), vm((R, d), F32), vm((R, d), BF), vm((R, d), BF), vm((1, d), F32), vm((R, HEAD), F32), vm((4, 1, d), F32), vm((1, d), F32),
                        pltpu.SemaphoreType.DMA((R // chunk, 5)), pltpu.SemaphoreType.DMA((R // chunk + 3,))],
        compiler_params=pltpu.CompilerParams(vmem_limit_bytes=62 * 2**20),
        cost_estimate=pl.CostEstimate(flops=16 * R * d, bytes_accessed=12 * R * d, transcendentals=R),
        name="close",
    )(x, dy, near, hi, lo, gain, scale, parts)


def solution(mesh):
    def step(x, dy, gain, wq, wk, wv, wo):
        a, dy_all, o, dq, dkv, near, hi, lo, gain_row, scale, parts = main(x, dy, gain, wq, wk, wv, wo)
        got = lax.ppermute(lo, "tp", [(0, 2), (2, 0)])
        by_wq, by_wk, by_wv, by_wo = weight_gradients(a, dq, dkv, o, dy_all)
        gain_row, by_wk = lax.optimization_barrier((gain_row, by_wk))
        by_x, by_gain = close(x, dy, near, hi, got, gain_row, scale, parts)
        return by_x, by_gain, by_wq, by_wk, by_wv, by_wo

    tokens, columns = P(("dp", "tp"), None), P(None, "tp")
    return jax.shard_map(
        step,
        mesh=mesh,
        in_specs=(tokens, tokens, P(None), columns, columns, columns, P("tp", None)),
        out_specs=(tokens, P("dp", None), P("dp", "tp"), P("dp", "tp"), P("dp", "tp"), P(("dp", "tp"), None)),
        check_vma=False,
    )
```
